512 devices in a mesh: row: 16 (over y_lo, x), col: 8 (over z), vol: 4 (over y_hi, core).
Axes of the slice: x: 4, y: 8 (y_hi: 2, y_lo: 4; y = y_hi * 4 + y_lo), z: 8, core: 2. Of those that a mesh axis runs over, the one named last changes fastest.
Arguments:
- panel: bfloat16 [2048, 131072], P('row', ('col', 'vol')), may hold values from -0.015625 to 0.015625
- density: float32 [32, 131072], P(None, ('col', 'vol')), may hold values from -6 to 6
- source: float32 [32, 128, 64, 512], P(None, 'row', 'col', 'vol'), may hold values from -6 to 6
- class_index: int32 [128, 64, 512], P('row', 'col', 'vol'), may hold values from 0 to 15
- class_values: float32 [16], replicated, may hold values from 0.2 to 5
- trace_count: int32 [16, 32], P('row'), may hold values from 1 to 16, 128 in all within a row
- trace_cell: int32 [16, 32, 16], P('row'), may hold values from 0 to 8191
Outputs:
- density_out: float32 [32, 131072], P(None, ('col', 'vol'))
- volume_out: float32 [32, 128, 64, 512], P(None, 'row', 'col', 'vol')
The draws below stay inside these ranges and needn't reach their ends.
Inputs may be any that keep to these rules, and one draw needn't show every extreme that they name: `trace_count`: in each row r, the counts of the 32 blocks are 1 or more and sum to 128, so that every target of row tile r has exactly one live slot; the largest count of each row is 16. `trace_cell`: only the first trace_count[r, j] slots of block j are read; two slots may hit one cell.
All inputs are finite; a program needn't handle non-finite values.
Results may differ from the reference program's by a relative error of at most 0.00035.
Values may be sent and summed in bfloat16 or wider, within the bound.
A program may use at most 128 MiB of HBM per device.

```python
import math
import jax
import jax.numpy as jnp
import numpy as np
from jax import lax

NS = 131072
E = 32
TGT_DEV = 128
CX = 8
CY = 8
CZ = 128
SWEEPS = 4
OUTER = 2
NCLASS = 16
BLOCKS = 32
SLOTS = 16
TGT = 2048
NX = 128
NY = 64
NZ = 512
N_ROW = 16
N_VOL = 4


def plant(values, key, low, high):
    longest = values.shape.index(max(values.shape))
    spots = []
    for shift in (0, 1):
        where = [jax.random.randint(jax.random.fold_in(key, axis), (), 0, length) for axis, length in enumerate(values.shape)]
        where[longest] = (where[longest] + shift) % values.shape[longest]
        spots.append(tuple(where))
    return values.at[spots[0]].set(low).at[spots[1]].set(high)


def levels(rng, shape, split, smallest, largest):
    def one(position, parts):
        heights = jax.random.uniform(jax.random.fold_in(jax.random.fold_in(rng, 6), position), (parts,), jnp.float32, smallest / len(split), largest / len(split))
        return jnp.repeat(jnp.exp(heights), shape[position] // parts).reshape((-1,) + (1,) * (len(shape) - position - 1))

    gain = one(*split[0])
    for cut in split[1:]:
        gain = gain * one(*cut)
    return gain


def split_up(number_of, total, limit, skew):
    loads = [(1 << 20) // math.isqrt(rank ** skew) + 1 for rank in range(2, number_of + 1)]
    rest, given = total - limit - (number_of - 1), [1] * (number_of - 1)
    while rest > 0:
        free = [i for i in range(number_of - 1) if given[i] < limit]
        mass, remaining = sum([loads[i] for i in free]), rest
        for i in free:
            extra = min(limit - given[i], max(1, remaining * loads[i] // mass), rest)
            given[i] = given[i] + extra
            rest = rest - extra
    return np.array([limit] + given)


def ragged_sizes(key, number_of, total, limit, lean):
    if number_of == 2:
        one = jax.random.randint(key, (), max(1, total - limit), min(limit, total - 1) + 1)
        return jnp.stack([one, total - one])
    tallies = jnp.asarray(split_up(number_of, total, limit, lean), jnp.int32)
    twos = (number_of - 1) // 2
    giver, taker = tallies[1:1 + 2 * twos:2], tallies[2:2 + 2 * twos:2]
    margin = jnp.minimum(giver - 1, limit - taker)
    moved = jax.random.randint(jax.random.fold_in(key, 1), (twos,), 0, 1 << 20) % (margin + 1)
    tallies = tallies.at[1:1 + 2 * twos:2].set(giver - moved).at[2:2 + 2 * twos:2].set(taker + moved)
    return tallies[jax.random.permutation(jax.random.fold_in(key, 2), number_of)]


def centred(rng, dims, scale, reach, cuts=(), kind=jnp.bfloat16):
    drawn = scale * jax.random.normal(rng, dims, jnp.float32)
    if cuts:
        drawn = drawn * levels(rng, dims, cuts, -0.22, 0.18)
    return jnp.clip(drawn, -reach, reach).astype(kind)


def setup_inputs(seed: int = 0) -> dict:
    key_of = jax.random.split(jax.random.key(seed), 8)
    panel = centred(key_of[0], (TGT, NS), NS ** -0.5, 0.015625, ((0, 16), (1, 32)))
    density = centred(key_of[1], (E, NS), 1.0, 6.0, ((1, 32),), jnp.float32)
    source = centred(key_of[2], (E, NX, NY, NZ), 1.0, 6.0, ((1, 16), (2, 8), (3, 4)), jnp.float32)
    class_index = plant(jax.random.randint(key_of[3], (NX, NY, NZ), 0, NCLASS), jax.random.fold_in(key_of[3], 1), 0, NCLASS - 1).astype(jnp.int32)
    class_values = jnp.clip(jnp.exp(jax.random.uniform(key_of[4], (NCLASS,), jnp.float32, math.log(0.2), math.log(5.0))), 0.2, 5.0)
    trace_count = jax.vmap(lambda own: ragged_sizes(own, BLOCKS, TGT_DEV, SLOTS, 2))(jax.random.split(key_of[5], N_ROW)).reshape((N_ROW, BLOCKS)).astype(jnp.int32)
    trace_cell = plant(jax.random.randint(key_of[6], (N_ROW, BLOCKS, SLOTS), 0, CX * CY * CZ), jax.random.fold_in(key_of[6], 1), 0, (CX * CY * CZ) - 1).astype(jnp.int32)
    return dict(panel=panel, density=density, source=source, class_index=class_index, class_values=class_values, trace_count=trace_count, trace_cell=trace_cell)


MASS_TERM = 0.1
RELAXATION = 0.5
SPECTRUM_LOW = 0.1
SPECTRUM_HIGH = 2.0


def relax_factors(count):
    middle = (SPECTRUM_HIGH + SPECTRUM_LOW) / 2.0
    spread = (SPECTRUM_HIGH - SPECTRUM_LOW) / 2.0
    return [1.0 / (middle + spread * math.cos(math.pi * (2 * order + 1) / (2 * count))) for order in range(count)]


def neighbours(padded):
    center = padded[..., 1:-1, 1:-1, 1:-1]
    beside_all = padded[..., 2:, 1:-1, 1:-1] + padded[..., :-2, 1:-1, 1:-1]
    beside_all = beside_all + padded[..., 1:-1, 2:, 1:-1] + padded[..., 1:-1, :-2, 1:-1]
    beside_all = beside_all + padded[..., 1:-1, 1:-1, 2:] + padded[..., 1:-1, 1:-1, :-2]
    return center, beside_all


def reference(panel, density, source, class_index, class_values, trace_count, trace_cell):
    conduct = jnp.take(class_values, class_index)
    diagonal = MASS_TERM + 6.0 * conduct
    offsets = jnp.cumsum(trace_count, axis=1) - trace_count
    slot_ids = jnp.arange(SLOTS, dtype=jnp.int32)
    live_slots = slot_ids[None, None, :] < trace_count[:, :, None]
    row_ids = jnp.arange(N_ROW, dtype=jnp.int32)[:, None, None]
    block_ids = jnp.arange(BLOCKS, dtype=jnp.int32)[None, :, None]
    targets = row_ids * TGT_DEV + jnp.minimum(offsets[:, :, None] + slot_ids[None, None, :], TGT_DEV - 1)
    col_place = block_ids // N_VOL
    vol_place = block_ids % N_VOL
    local_x = trace_cell // (CY * CZ)
    local_y = (trace_cell // CZ) % CY
    local_z = trace_cell % CZ
    global_cell = ((row_ids * CX + local_x) * NY + col_place * CY + local_y) * NZ + vol_place * CZ + local_z
    targets = targets.reshape(-1).astype(jnp.int32)
    global_cell = global_cell.reshape(-1).astype(jnp.int32)
    weights = live_slots.reshape(-1).astype(jnp.float32)
    factors = relax_factors(SWEEPS)

    def relax_one(pair):
        volume, right_side = pair
        for factor in factors:
            padded = jnp.pad(volume, 1)
            center, beside_all = neighbours(padded)
            volume = center + factor * (right_side - diagonal * center + conduct * beside_all) / diagonal
        return volume

    volume = jnp.zeros(source.shape, jnp.float32)
    for iteration in range(OUTER):
        rounded = density.astype(jnp.bfloat16)
        potential = jnp.dot(rounded, panel.T, preferred_element_type=jnp.float32)
        slot_values = potential[:, targets] * weights
        right_side = source.reshape(E, -1).at[:, global_cell].add(slot_values).reshape(source.shape)
        volume = lax.map(relax_one, (volume, right_side))
        mismatch = (volume.reshape(E, -1)[:, global_cell] - slot_values) * weights
        fluxes = jnp.zeros((E, TGT), jnp.float32).at[:, targets].add(mismatch)
        update = jnp.dot(fluxes.astype(jnp.bfloat16), panel, preferred_element_type=jnp.float32)
        density = density + RELAXATION * update
    return density, volume
```

```python
import functools
import math

import jax
import jax.numpy as jnp
from jax import lax
from jax.experimental import pallas as pl
from jax.experimental.pallas import tpu as pltpu
from jax.sharding import PartitionSpec as P

SWEEPS = 4
OUTER = 2
MASS_TERM = 0.1
RELAXATION = 0.5
SPECTRUM_LOW = 0.1
SPECTRUM_HIGH = 2.0
MESH = pl.DeviceIdType.MESH
F32 = jnp.float32
BF16 = jnp.bfloat16
GROUP = 16
NT = (((1,), (1,)), ((), ()))


def relax_factors(count):
    middle = (SPECTRUM_HIGH + SPECTRUM_LOW) / 2.0
    spread = (SPECTRUM_HIGH - SPECTRUM_LOW) / 2.0
    return [
        1.0 / (middle + spread * math.cos(math.pi * (2 * order + 1) / (2 * count)))
        for order in range(count)
    ]


def kernel(
    sizes,
    panel, density, source, class_index, class_values, target_of, cell_of,
    density_out, volume_out,
    select, hot, spots, conduct, inverse, base, field, xlo, xhi, ylo, yhi, zlo, zhi,
    yface, zface, zmix, slot, picked, psend, pbuf, fsend, fbuf, fall, strip, dsend, rbuf, osend,
    halo_send, halo_recv, phase_send, phase_recv,
):
    n_row, n_col, n_vol = sizes
    blocks = n_col * n_vol
    columns = blocks // 8
    share = density.shape[1] // n_row
    lead = source.shape[0]
    high = lead // 8
    factors = relax_factors(SWEEPS)
    row = lax.axis_index("row")
    col = lax.axis_index("col")
    vol = lax.axis_index("vol")
    me = col * n_vol + vol

    def block_id(j):
        return {"col": j // n_vol, "vol": j % n_vol}

    def block_peer(d):
        return lax.rem(me + d, blocks)

    def row_peer(d):
        return lax.rem(row + d, n_row)

    barrier = pltpu.get_barrier_semaphore()

    @pl.loop(1, blocks)
    def _(d):
        pl.semaphore_signal(barrier, inc=1, device_id=block_id(block_peer(d)), device_id_type=MESH)

    @pl.loop(1, n_row)
    def _(d):
        pl.semaphore_signal(barrier, inc=1, device_id={"row": row_peer(d)}, device_id_type=MESH)

    def remote(src, dst, send, recv, device):
        return pltpu.make_async_remote_copy(
            src_ref=src, dst_ref=dst, send_sem=send, recv_sem=recv,
            device_id=device, device_id_type=MESH,
        )

    def whole(ref, phase):
        return remote(ref, ref, phase_send.at[phase], phase_recv.at[phase], {"row": row})

    sub = lax.broadcasted_iota(jnp.int32, (8, 128), 0)
    lane = lax.broadcasted_iota(jnp.int32, (8, 128), 1)
    group = lane // GROUP

    rows_t = lax.broadcasted_iota(jnp.int32, select.shape, 0)
    select[...] = jnp.where(rows_t == target_of[0:1, :], 1.0, 0.0).astype(F32)
    cells = cell_of[0:1, :]
    hot_z = lax.broadcasted_iota(jnp.int32, hot.shape, 0)
    hot[...] = jnp.where(hot_z == cells % 128, 1.0, 0.0).astype(F32)
    spot_rows = lax.broadcasted_iota(jnp.int32, (64, 128), 0)
    spot_lane = lax.broadcasted_iota(jnp.int32, (64, 128), 1)
    part = lax.rem(spot_lane // GROUP - lax.rem(me, 8) + 8, 8)
    hit = (spot_rows == cells // 128) & (cells >= 0)
    for h in range(high):
        spots[h] = jnp.where(hit & (part == h), 1.0, 0.0).astype(F32)
    cls = class_index[...]
    value = jnp.zeros(cls.shape, F32)
    for k in range(class_values.shape[0]):
        value = jnp.where(cls == k, class_values[k], value)
    diagonal = MASS_TERM + 6.0 * value
    conduct[...] = value / diagonal
    inverse[...] = 1.0 / diagonal

    exchanges = xlo.shape[0]

    def clear(ref):
        @pl.loop(0, exchanges)
        def _(k):
            ref[k] = jnp.zeros(ref.shape[1:], F32)

    for here, edge, ref in (
        (row, 0, xlo), (row, n_row - 1, xhi), (col, 0, ylo),
        (col, n_col - 1, yhi), (vol, 0, zlo), (vol, n_vol - 1, zhi),
    ):
        @pl.when(here == edge)
        def _(ref=ref):
            clear(ref)

    def send_potential(it, chunk):
        partial = jnp.zeros((lead, panel.shape[0]), F32)
        for k in range(n_row):
            partial += lax.dot_general(
                chunk(k), panel[:, k * share : (k + 1) * share], NT, preferred_element_type=F32
            )
        chosen = jnp.dot(
            partial, select[...], precision=lax.Precision.HIGHEST, preferred_element_type=F32
        )
        for g in range(columns):
            turned = [
                pltpu.roll(
                    chosen[8 * h : 8 * h + 8, 128 * g : 128 * g + 128], (GROUP * h) % 128, 1
                )
                for h in range(high)
            ]
            for d in range(8):
                tile = jnp.zeros((8, 128), F32)
                for h in range(high):
                    tile = jnp.where(group == (d + h) % 8, turned[h], tile)
                psend[it, g * 8 + d] = tile
        if it == 0:
            pl.semaphore_wait(barrier, blocks - 1 + n_row - 1)
        pbuf[it, me] = psend[it, me]

        @pl.loop(1, blocks)
        def _(d):
            j = block_peer(d)
            remote(
                psend.at[it, j], pbuf.at[it, me], phase_send.at[it], phase_recv.at[it], block_id(j)
            ).start()

    def right_side(it):
        whole(pbuf.at[it, pl.ds(0, blocks - 1)], it).wait_recv()
        total = pbuf[it, 0]
        for j in range(1, blocks):
            total += pbuf[it, j]
        slot[...] = total

        def build(low, carry):
            for h in range(high):
                spread = slot[pl.ds(low, 1), :] * spots[h]
                added = lax.dot_general(
                    spread, hot[...], NT, precision=lax.Precision.HIGHEST,
                    preferred_element_type=F32,
                )
                e = h * 8 + low
                base[e] = (source[e] + added) * inverse[...]
            return carry

        lax.fori_loop(0, 8, build, 0)

    def faces(slot_index, e, new, packed):
        out = []
        for x in range(8):
            moved = pltpu.roll(new[x], lax.rem(2 * e, 128), 1)
            ours = (lane == 2 * e) | (lane == lax.rem(2 * e + 127, 128))
            out.append(jnp.where(ours, moved, packed[x]))
        yface[slot_index, 0, e] = field[slot_index, e, pl.ds(0, 8, stride=8), :]
        yface[slot_index, 1, e] = field[slot_index, e, pl.ds(7, 8, stride=8), :]
        return out

    def first_sweep(out_index, factor):
        def step(e, packed):
            new = [factor * base[e, 8 * x : 8 * x + 8, :] for x in range(8)]
            for x in range(8):
                field[out_index, e, 8 * x : 8 * x + 8, :] = new[x]
            return faces(out_index, e, new, packed)

        packed = lax.fori_loop(0, lead, step, [jnp.zeros((8, 128), F32)] * 8)
        for x in range(8):
            zface[out_index, x] = packed[x]

    def halo_copies(k):
        return (
            (row < n_row - 1, remote(field.at[k, :, pl.ds(56, 8), :], xlo.at[k], halo_send.at[k, 0], halo_recv.at[k, 0], {"row": row + 1})),
            (row > 0, remote(field.at[k, :, pl.ds(0, 8), :], xhi.at[k], halo_send.at[k, 1], halo_recv.at[k, 1], {"row": row - 1})),
            (col < n_col - 1, remote(yface.at[k, 1], ylo.at[k], halo_send.at[k, 2], halo_recv.at[k, 2], {"col": col + 1})),
            (col > 0, remote(yface.at[k, 0], yhi.at[k], halo_send.at[k, 3], halo_recv.at[k, 3], {"col": col - 1})),
            (vol < n_vol - 1, remote(zface.at[k], zlo.at[k], halo_send.at[k, 4], halo_recv.at[k, 4], {"vol": vol + 1})),
            (vol > 0, remote(zface.at[k], zhi.at[k], halo_send.at[k, 5], halo_recv.at[k, 5], {"vol": vol - 1})),
        )

    arrives = (row > 0, row < n_row - 1, col > 0, col < n_col - 1, vol > 0, vol < n_vol - 1)

    def halo_start(k):
        copies = halo_copies(k)
        for i in (4, 5, 0, 1, 2, 3):
            @pl.when(copies[i][0])
            def _(copy=copies[i][1]):
                copy.start()

    def halo_wait(k):
        for i, (_, copy) in enumerate(halo_copies(k)):
            @pl.when(arrives[i])
            def _(copy=copy):
                copy.wait_recv()

    def halo_sent(k):
        for go, copy in halo_copies(k):
            @pl.when(go)
            def _(copy=copy):
                copy.wait_send()

    def sweep(k, factor, last):
        halo_wait(k)
        odd = lax.rem(lane, 2) == 1
        for x in range(8):
            zmix[x] = jnp.where(odd, pltpu.roll(zlo[k, x], 2, 1), zhi[k, x])

        def step(e, packed):
            old = [field[k, e, 8 * x : 8 * x + 8, :] for x in range(8)]
            new = []
            turn = lax.rem(127 - 2 * e + 128, 128)
            for x in range(8):
                c = old[x]
                below = xlo[k, e] if x == 0 else old[x - 1]
                above = xhi[k, e] if x == 7 else old[x + 1]
                left = jnp.where(sub == 0, ylo[k, e, x : x + 1, :], pltpu.roll(c, 1, 0))
                right = jnp.where(sub == 7, yhi[k, e, x : x + 1, :], pltpu.roll(c, 7, 0))
                ends = pltpu.roll(zmix[x], turn, 1)
                front = jnp.where(lane == 0, ends, pltpu.roll(c, 1, 1))
                back = jnp.where(lane == 127, ends, pltpu.roll(c, 127, 1))
                around = (below + above) + (left + right) + (front + back)
                span = slice(8 * x, 8 * x + 8)
                n = (1.0 - factor) * c + factor * (base[e, span, :] + conduct[span, :] * around)
                if last:
                    volume_out[e, span, :] = n
                else:
                    field[k + 1, e, span, :] = n
                new.append(n)
            if last:
                return packed
            return faces(k + 1, e, new, packed)

        if last:
            lax.fori_loop(0, lead, step, 0)
        else:
            packed = lax.fori_loop(0, lead, step, [jnp.zeros((8, 128), F32)] * 8)
            for x in range(8):
                zface[k + 1, x] = packed[x]

    def send_flux(it, read):
        def pick(low, carry):
            total = jnp.zeros((8, 128), F32)
            for h in range(high):
                seen = jnp.dot(
                    read(h * 8 + low), hot[...], precision=lax.Precision.HIGHEST,
                    preferred_element_type=F32,
                ) * spots[h]
                for x in range(8):
                    total += seen[8 * x : 8 * x + 8, :]
            picked[pl.ds(low, 1), :] = jnp.sum(total, axis=0, keepdims=True)
            return carry

        lax.fori_loop(0, 8, pick, 0)
        flux = picked[...] - slot[...]
        fsend[it] = flux
        fbuf[it, me] = flux

        @pl.loop(1, blocks)
        def _(d):
            remote(
                fsend.at[it], fbuf.at[it, me], phase_send.at[2 + it], phase_recv.at[2 + it],
                block_id(block_peer(d)),
            ).start()

    def spread_flux(it):
        whole(fbuf.at[it, pl.ds(0, blocks - 1)], 2 + it).wait_recv()
        dense = jnp.zeros((lead, panel.shape[0]), F32)
        for g in range(columns):
            parts = []
            for h in range(high):
                mixed = fbuf[it, g * 8]
                for d in range(1, 8):
                    mixed = jnp.where(group == (d + h) % 8, fbuf[it, g * 8 + d], mixed)
                parts.append(pltpu.roll(mixed, (128 - GROUP * h) % 128, 1))
            block = jnp.concatenate(parts, axis=0).astype(BF16)
            dense += lax.dot_general(
                block, select[:, 128 * g : 128 * g + 128].astype(BF16), NT,
                preferred_element_type=F32,
            )
        fall[it, row] = dense.astype(BF16)

        @pl.loop(1, n_row)
        def _(d):
            remote(
                fall.at[it, row], fall.at[it, row], phase_send.at[4 + it], phase_recv.at[4 + it],
                {"row": row_peer(d)},
            ).start()

    def panel_copy(d):
        r = row_peer(d)
        return remote(
            panel.at[:, pl.ds(pl.multiple_of(r * share, share), share)], strip.at[row],
            phase_send.at[6], phase_recv.at[6], {"row": r},
        )

    def send_panel(first, count):
        @pl.loop(first, min(first + count, n_row))
        def _(d):
            panel_copy(d).start()

    def new_share(it, old):
        whole(fall.at[it, pl.ds(0, n_row - 1)], 4 + it).wait_recv()
        if it == 0:
            whole(strip.at[pl.ds(0, n_row - 1)], 6).wait_recv()
        update = jnp.zeros((lead, share), F32)
        for r in range(n_row):
            update += jnp.dot(fall[it, r], strip[r], preferred_element_type=F32)
        return old + RELAXATION * update

    own = pl.ds(pl.multiple_of(row * share, share), share)

    send_potential(0, lambda k: density[:, k * share : (k + 1) * share].astype(BF16))
    strip[row] = panel[:, own]
    send_panel(1, 4)
    right_side(0)
    first_sweep(0, factors[0])
    halo_start(0)
    send_panel(5, 4)
    sweep(0, factors[1], False)
    halo_start(1)
    send_panel(9, 4)
    sweep(1, factors[2], False)
    halo_start(2)
    send_panel(13, n_row)
    sweep(2, factors[3], False)
    send_flux(0, lambda e: field[3, e])
    halo_start(3)
    spread_flux(0)
    state = new_share(0, density[:, own])
    osend[0] = state
    rounded = state.astype(BF16)
    dsend[...] = rounded
    rbuf[row] = rounded

    @pl.loop(1, n_row)
    def _(d):
        remote(
            dsend, rbuf.at[row], phase_send.at[7], phase_recv.at[7], {"row": row_peer(d)}
        ).start()

    whole(rbuf.at[pl.ds(0, n_row - 1)], 7).wait_recv()

    send_potential(1, lambda k: rbuf[k])
    right_side(1)
    sweep(3, factors[0], False)
    halo_start(4)
    sweep(4, factors[1], False)
    halo_start(5)
    sweep(5, factors[2], False)
    halo_start(6)
    sweep(6, factors[3], True)
    send_flux(1, lambda e: volume_out[e])
    spread_flux(1)
    state = new_share(1, osend[0])
    osend[1] = state
    density_out[:, own] = state

    @pl.loop(1, n_row)
    def _(d):
        remote(
            osend.at[1], density_out.at[:, own], phase_send.at[8], phase_recv.at[8],
            {"row": row_peer(d)},
        ).start()

    whole(density_out.at[:, pl.ds(0, (n_row - 1) * share)], 8).wait_recv()

    for it in range(OUTER):
        whole(pbuf.at[it, pl.ds(0, blocks - 1)], it).wait_send()
        whole(fbuf.at[it, pl.ds(0, blocks - 1)], 2 + it).wait_send()
        whole(fall.at[it, pl.ds(0, n_row - 1)], 4 + it).wait_send()
    whole(strip.at[pl.ds(0, n_row - 1)], 6).wait_send()
    whole(rbuf.at[pl.ds(0, n_row - 1)], 7).wait_send()
    whole(density_out.at[:, pl.ds(0, (n_row - 1) * share)], 8).wait_send()
    for k in range(exchanges):
        halo_sent(k)


def local(panel, density, source, class_index, class_values, trace_count, trace_cell):
    sizes = (lax.axis_size("row"), lax.axis_size("col"), lax.axis_size("vol"))
    n_row, n_col, n_vol = sizes
    blocks = n_col * n_vol
    lead = source.shape[0]
    targets, nodes = panel.shape
    share = nodes // n_row
    slots = trace_cell.shape[2]
    counts = trace_count[0]
    offsets = jnp.cumsum(counts) - counts
    slot_ids = jnp.arange(slots, dtype=jnp.int32)
    live = slot_ids[None, :] < counts[:, None]
    target_of = jnp.where(live, offsets[:, None] + slot_ids[None, :], -1)
    target_of = jnp.broadcast_to(target_of.reshape(1, blocks * slots), (8, blocks * slots))
    block_index = lax.axis_index(("col", "vol"))
    cells = jnp.where(live, trace_cell[0], -1)
    cells = lax.dynamic_index_in_dim(cells, block_index, keepdims=False)
    cell_of = jnp.broadcast_to(cells[None, None, :], (8, 8, slots)).reshape(8, 8 * slots)
    exchanges = SWEEPS * OUTER - 1
    vmem = lambda shape, kind=F32: pltpu.VMEM(shape, kind)
    dma = pltpu.SemaphoreType.DMA
    density_out, volume = pl.pallas_call(
        functools.partial(kernel, sizes),
        out_shape=(
            jax.ShapeDtypeStruct(density.shape, F32),
            jax.ShapeDtypeStruct((lead, 64, 128), F32),
        ),
        in_specs=[
            pl.BlockSpec(memory_space=pltpu.VMEM),
            pl.BlockSpec(memory_space=pltpu.VMEM),
            pl.BlockSpec(memory_space=pltpu.VMEM),
            pl.BlockSpec(memory_space=pltpu.VMEM),
            pl.BlockSpec(memory_space=pltpu.SMEM),
            pl.BlockSpec(memory_space=pltpu.VMEM),
            pl.BlockSpec(memory_space=pltpu.VMEM),
        ],
        out_specs=(
            pl.BlockSpec(memory_space=pltpu.VMEM),
            pl.BlockSpec(memory_space=pltpu.VMEM),
        ),
        scratch_shapes=[
            vmem((targets, blocks * slots)),
            vmem((128, 128)),
            vmem((lead // 8, 64, 128)),
            vmem((64, 128)),
            vmem((64, 128)),
            vmem((lead, 64, 128)),
            vmem((exchanges, lead, 64, 128)),
            vmem((exchanges, lead, 8, 128)),
            vmem((exchanges, lead, 8, 128)),
            vmem((exchanges, lead, 8, 128)),
            vmem((exchanges, lead, 8, 128)),
            vmem((exchanges, 8, 8, 128)),
            vmem((exchanges, 8, 8, 128)),
            vmem((exchanges, 2, lead, 8, 128)),
            vmem((exchanges, 8, 8, 128)),
            vmem((8, 8, 128)),
            vmem((8, 128)),
            vmem((8, 128)),
            vmem((OUTER, blocks, 8, 128)),
            vmem((OUTER, blocks, 8, 128)),
            vmem((OUTER, 8, 128)),
            vmem((OUTER, blocks, 8, 128)),
            vmem((OUTER, n_row, lead, targets), BF16),
            vmem((n_row, targets, share), BF16),
            vmem((lead, share), BF16),
            vmem((n_row, lead, share), BF16),
            vmem((OUTER, lead, share)),
            dma((exchanges, 6)),
            dma((exchanges, 6)),
            dma((9,)),
            dma((9,)),
        ],
        compiler_params=pltpu.CompilerParams(
            collective_id=0, has_side_effects=True, vmem_limit_bytes=56 * 1024 * 1024
        ),
    )(
        panel,
        density,
        source.reshape(lead, 64, 128),
        class_index.reshape(64, 128),
        class_values,
        target_of,
        cell_of,
    )
    return density_out, volume.reshape(source.shape)


def solution(mesh):
    placed = (
        P("row", ("col", "vol")),
        P(None, ("col", "vol")),
        P(None, "row", "col", "vol"),
        P("row", "col", "vol"),
        P(),
        P("row", None),
        P("row", None, None),
    )
    return jax.shard_map(
        local,
        mesh=mesh,
        in_specs=placed,
        out_specs=(P(None, ("col", "vol")), P(None, "row", "col", "vol")),
        check_vma=False,
    )
```

```python
import functools
import math

import jax
import jax.numpy as jnp
from jax import lax
from jax.experimental import pallas as pl
from jax.experimental.pallas import tpu as pltpu
from jax.sharding import PartitionSpec as P

SWEEPS = 4
OUTER = 2
MASS_TERM = 0.1
RELAXATION = 0.5
SPECTRUM_LOW = 0.1
SPECTRUM_HIGH = 2.0
MESH = pl.DeviceIdType.MESH
F32 = jnp.float32
BF16 = jnp.bfloat16
NT = (((1,), (1,)), ((), ()))
TN = (((0,), (0,)), ((), ()))
SLOTS = 16
TURN = 4
SPANS = tuple(slice(8 * b, 8 * b + 8) for b in range(4))


def relax_factors(count):
    middle = (SPECTRUM_HIGH + SPECTRUM_LOW) / 2.0
    spread = (SPECTRUM_HIGH - SPECTRUM_LOW) / 2.0
    return [
        1.0 / (middle + spread * math.cos(math.pi * (2 * order + 1) / (2 * count)))
        for order in range(count)
    ]


def kernel(
    sizes,
    panel, density, source, class_index, class_values, trace_count, trace_cell,
    density_out, volume_out,
    select, hits, conduct, inverse, inner, middle, base, field, zface, zlo, zhi, zrow, zmix,
    turned, slot, picked, psend, pbuf, fsend, fbuf, fall, strip, rbuf, osend,
    halo_send, halo_recv, phase_send, phase_recv,
):
    n_row, n_col, n_vol = sizes
    blocks = n_col * n_vol
    share = density.shape[1] // n_row
    lead = density.shape[0]
    factors = relax_factors(SWEEPS)
    row = lax.axis_index("row")
    col = lax.axis_index("col")
    vol = lax.axis_index("vol")
    me = col * n_vol + vol

    def block_id(j):
        return {"col": j // n_vol, "vol": j % n_vol}

    def block_peer(d):
        return lax.rem(me + d, blocks)

    def row_peer(d):
        return lax.rem(row + d, n_row)

    barrier = pltpu.get_barrier_semaphore()

    @pl.loop(1, blocks)
    def _(d):
        pl.semaphore_signal(barrier, inc=1, device_id=block_id(block_peer(d)), device_id_type=MESH)

    @pl.loop(1, n_row)
    def _(d):
        pl.semaphore_signal(barrier, inc=1, device_id={"row": row_peer(d)}, device_id_type=MESH)

    def remote(src, dst, send, recv, device):
        return pltpu.make_async_remote_copy(
            src_ref=src, dst_ref=dst, send_sem=send, recv_sem=recv,
            device_id=device, device_id_type=MESH,
        )

    def whole(ref, phase):
        return remote(ref, ref, phase_send.at[phase], phase_recv.at[phase], {"row": row})

    sub = lax.broadcasted_iota(jnp.int32, (8, 128), 0)
    lane = lax.broadcasted_iota(jnp.int32, (8, 128), 1)
    group = lane // 32
    exchanges = field.shape[0]

    def pieces(x):
        first = x.astype(BF16)
        rest = x - first.astype(F32)
        second = rest.astype(BF16)
        third = (rest - second.astype(F32)).astype(BF16)
        return first, second, third

    offset = jnp.int32(0)
    marks = []
    for j in range(blocks):
        count = trace_count[0, j]
        marks.append((offset, count))
        offset = offset + count
    for p in range(2):
        for j in range(0, blocks, 2):
            both = []
            for start, count in marks[j : j + 2]:
                s = sub + 8 * p
                both.append(jnp.where((lane == s + start) & (s < count), 1.0, 0.0).astype(F32))
            at = p * blocks * 8 + j * 8
            select[at : at + 16, :] = jnp.concatenate(both, axis=0).astype(BF16)

    def quarters(tiles):
        a = list(tiles)
        grp = lax.broadcasted_iota(jnp.int32, a[0].shape, 1) // 32
        for step in (2, 1):
            out = list(a)
            for i in range(4):
                if i & step == 0:
                    j = i | step
                    shift = 32 * step
                    keep = (grp & step) == 0
                    out[i] = jnp.where(keep, a[i], pltpu.roll(a[j], shift, 1))
                    out[j] = jnp.where(keep, pltpu.roll(a[i], 128 - shift, 1), a[j])
            a = out
        return a

    def to_inner(rows, write):
        @pl.loop(0, 16, unroll=TURN)
        def _(i):
            x, y = i // 2, (i % 2) * 4
            stacked = jnp.concatenate([rows(x, y + q) for q in range(4)], axis=0)
            flipped = jnp.transpose(stacked)
            for q, tile in enumerate(quarters([flipped[32 * q : 32 * q + 32, :] for q in range(4)])):
                write(x, y + q, tile)

    cls = class_index[...]
    value = jnp.zeros(cls.shape, F32)
    for k in range(class_values.shape[0]):
        value = jnp.where(cls == k, class_values[k], value)
    turned[...] = value

    def coefficients(x, y, tile):
        inv = 1.0 / (MASS_TERM + 6.0 * tile)
        inverse[x, y] = inv
        conduct[x, y] = tile * inv

    def prepare():
        to_inner(
            lambda x, y: jnp.broadcast_to(turned[pl.ds(x * 8 + y, 1), :], (lead, 128)), coefficients
        )

    def send_potential(it, chunk):
        partial = jnp.zeros((panel.shape[0], 128), F32)
        for k in range(n_row):
            part = chunk(k)
            partial += lax.dot_general(
                panel[:, k * share : (k + 1) * share],
                jnp.concatenate([part] * (128 // lead), axis=0),
                NT, preferred_element_type=F32,
            )
        chosen = jnp.zeros((select.shape[0], 128), F32)
        for piece in pieces(partial):
            chosen += jnp.dot(select[...], piece, preferred_element_type=F32)
        half = blocks * 8
        for j in range(blocks):
            psend[it, j] = jnp.where(
                group % 2 == 0, chosen[8 * j : 8 * j + 8, :],
                chosen[half + 8 * j : half + 8 * j + 8, :],
            )
        if it == 0:
            prepare()
            pl.semaphore_wait(barrier, blocks - 1 + n_row - 1)
        pbuf[it, me] = psend[it, me]

        @pl.loop(1, blocks)
        def _(d):
            j = block_peer(d)
            remote(
                psend.at[it, j], pbuf.at[it, me], phase_send.at[it], phase_recv.at[it], block_id(j)
            ).start()

    def panel_copy(d):
        r = row_peer(d)
        return remote(
            panel.at[:, pl.ds(pl.multiple_of(r * share, share), share)], strip.at[row],
            phase_send.at[6], phase_recv.at[6], {"row": r},
        )

    def send_panel(first, count):
        @pl.loop(first, min(first + count, n_row))
        def _(d):
            panel_copy(d).start()

    own = pl.ds(pl.multiple_of(row * share, share), share)
    send_potential(0, lambda k: density[:, k * share : (k + 1) * share].astype(BF16))
    strip[row] = panel[:, own]
    send_panel(1, 4)

    own_count = trace_count[0, me]
    cells, spot = [], jnp.full((8, 128), -1, jnp.int32)
    quarter = [jnp.full((8, 128), -1, jnp.int32) for _ in range(2)]
    for s in range(SLOTS):
        cell = jnp.where(s < own_count, trace_cell[0, me, s], -1)
        place = (cell >> 7) * 32 + (cell & 31)
        spot = jnp.where(lane % SLOTS == s, jnp.where(cell >= 0, place, -1), spot)
        fourth = jnp.where(cell >= 0, (cell >> 5) & 3, -1)
        quarter[s // 8] = jnp.where(sub == s % 8, fourth, quarter[s // 8])
        cells.append(jnp.maximum(place, 0))
    mine = [jnp.where(quarter[p] == group, 1.0, 0.0).astype(F32) for p in range(2)]
    spot = jnp.where(lane < 3 * SLOTS, spot, -1)

    @pl.loop(0, 128)
    def _(i):
        at = pl.multiple_of(i * 16, 16)
        here = jnp.concatenate([sub, sub + 8], axis=0) + at
        wide = jnp.concatenate([spot, spot], axis=0)
        hits[pl.ds(at, 16), :] = jnp.where(here == wide, 1.0, 0.0).astype(BF16)

    def keep_source(x, y, tile):
        inner[x, y] = tile

    to_inner(lambda x, y: source[pl.ds(x * 8 + y, lead, stride=64), :], keep_source)

    def clear(write):
        @pl.loop(0, exchanges)
        def _(k):
            write(k)

    def clear_x(k, x):
        field[k, x] = jnp.zeros(field.shape[2:], F32)

    def clear_y(k, y):
        @pl.loop(0, 10)
        def _(x):
            field[k, x, y] = jnp.zeros(field.shape[3:], F32)

    def clear_z(ref, k):
        ref[k] = jnp.zeros(ref.shape[1:], F32)

    for here, edge, write in (
        (row, 0, lambda k: clear_x(k, 0)), (row, n_row - 1, lambda k: clear_x(k, 9)),
        (col, 0, lambda k: clear_y(k, 0)), (col, n_col - 1, lambda k: clear_y(k, 9)),
        (vol, 0, lambda k: clear_z(zlo, k)), (vol, n_vol - 1, lambda k: clear_z(zhi, k)),
    ):
        @pl.when(here == edge)
        def _(write=write):
            clear(write)

    def right_side(it):
        whole(pbuf.at[it, pl.ds(0, blocks - 1)], it).wait_recv()
        total = pbuf[it, 0]
        for j in range(1, blocks):
            total += pbuf[it, j]
        swapped = pltpu.roll(total, 32, 1)
        even = group % 2 == 0
        parts = [jnp.where(even, total, swapped), jnp.where(even, swapped, total)]
        for p in range(2):
            slot[p] = parts[p]
        placed = jnp.concatenate([parts[p] * mine[p] for p in range(2)], axis=0)
        values = jnp.concatenate(
            list(pieces(placed)) + [jnp.zeros((128 - 3 * SLOTS, 128), BF16)], axis=0
        )

        @pl.loop(0, 8)
        def _(x):
            at = pl.multiple_of(x * 256, 256)
            added = jnp.dot(hits[pl.ds(at, 256), :], values, preferred_element_type=F32)
            for y in range(8):
                base[x, y] = (inner[x, y] + added[32 * y : 32 * y + 32, :]) * inverse[x, y]

    def keep(k, x, y, new, packed):
        low, top = packed
        for b in range(4):
            field[k, x + 1, y + 1, SPANS[b], :] = new[b]
        low = jnp.where(sub == y, pltpu.roll(new[0], y, 0) if y else new[0], low)
        top = jnp.where(sub == y, pltpu.roll(new[3], y + 1, 0) if y < 7 else new[3], top)
        return low, top

    def pack_rows(k):
        for side, edge in ((0, 0), (1, 3)):
            for b in range(2):
                packed = jnp.zeros((8, 128), F32)
                for i in range(4):
                    moved = zrow[k, side, 4 * b + i]
                    if i != edge:
                        moved = pltpu.roll(moved, (32 * (i - edge)) % 128, 1)
                    packed = jnp.where(group == i, moved, packed)
                zface[k, side, b] = packed

    def first_sweep(k, factor):
        @pl.loop(0, 8)
        def _(x):
            packed = (jnp.zeros((8, 128), F32),) * 2
            for y in range(8):
                new = [factor * base[x, y, SPANS[b], :] for b in range(4)]
                packed = keep(k, x, y, new, packed)
            zrow[k, 0, x], zrow[k, 1, x] = packed

        pack_rows(k)

    def halo_copies(k):
        pairs = (
            (row < n_row - 1, field.at[k, 8, pl.ds(1, 8)], field.at[k, 0, pl.ds(1, 8)], {"row": row + 1}),
            (row > 0, field.at[k, 1, pl.ds(1, 8)], field.at[k, 9, pl.ds(1, 8)], {"row": row - 1}),
            (col < n_col - 1, field.at[k, pl.ds(1, 8), 8], field.at[k, pl.ds(1, 8), 0], {"col": col + 1}),
            (col > 0, field.at[k, pl.ds(1, 8), 1], field.at[k, pl.ds(1, 8), 9], {"col": col - 1}),
            (vol < n_vol - 1, zface.at[k, 1], zlo.at[k], {"vol": vol + 1}),
            (vol > 0, zface.at[k, 0], zhi.at[k], {"vol": vol - 1}),
        )
        return [
            (go, remote(src, dst, halo_send.at[k, i], halo_recv.at[k, i], device))
            for i, (go, src, dst, device) in enumerate(pairs)
        ]

    arrives = (row > 0, row < n_row - 1, col > 0, col < n_col - 1, vol > 0, vol < n_vol - 1)

    def halo_start(k):
        copies = halo_copies(k)
        for i in (4, 5, 0, 1, 2, 3):
            @pl.when(copies[i][0])
            def _(copy=copies[i][1]):
                copy.start()

    def halo_wait(k):
        for i, (_, copy) in enumerate(halo_copies(k)):
            @pl.when(arrives[i])
            def _(copy=copy):
                copy.wait_recv()

    def halo_sent(k):
        for go, copy in halo_copies(k):
            @pl.when(go)
            def _(copy=copy):
                copy.wait_send()

    def sweep(k, factor, last, seen=None):
        halo_wait(k)
        for x in range(8):
            b, i = x // 4, x % 4
            low, top = zlo[k, b], zhi[k, b]
            low = pltpu.roll(low, 32 * (3 - i), 1) if i < 3 else low
            top = pltpu.roll(top, (128 - 32 * i) % 128, 1) if i else top
            zmix[0, x] = pltpu.roll(jnp.where(group == 3, low, zrow[k, 1, x]), 32, 1)
            zmix[1, x] = pltpu.roll(jnp.where(group == 0, top, zrow[k, 0, x]), 96, 1)

        @pl.loop(0, 8)
        def _(x):
            packed = (jnp.zeros((8, 128), F32),) * 2
            for y in range(8):
                c = [field[k, x + 1, y + 1, SPANS[b], :] for b in range(4)]
                ups = [pltpu.roll(v, 1, 0) for v in c]
                downs = [pltpu.roll(v, 7, 0) for v in c]
                new = []
                for b in range(4):
                    before = zmix[0, x, y : y + 1, :] if b == 0 else ups[b - 1]
                    after = zmix[1, x, y : y + 1, :] if b == 3 else downs[b + 1]
                    up = jnp.where(sub == 0, before, ups[b])
                    down = jnp.where(sub == 7, after, downs[b])
                    sp = SPANS[b]
                    around = (
                        (field[k, x, y + 1, sp, :] + field[k, x + 2, y + 1, sp, :])
                        + (field[k, x + 1, y, sp, :] + field[k, x + 1, y + 2, sp, :])
                        + (up + down)
                    )
                    new.append(
                        (1.0 - factor) * c[b]
                        + factor * (base[x, y, sp, :] + conduct[x, y, sp, :] * around)
                    )
                if seen is not None:
                    for b in range(4):
                        seen[x, y, SPANS[b], :] = new[b]
                if not last:
                    packed = keep(k + 1, x, y, new, packed)
            if not last:
                zrow[k + 1, 0, x], zrow[k + 1, 1, x] = packed

        if not last:
            pack_rows(k + 1)

    def send_flux(it, ref):
        for s in range(SLOTS):
            place = cells[s]
            picked[s : s + 1, :] = ref[
                place >> 8, (place >> 5) & 7, pl.ds(place & 31, 1), :
            ]
        fluxes = []
        for p in range(2):
            seen = picked[8 * p : 8 * p + 8, :] * mine[p]
            seen = seen + pltpu.roll(seen, 64, 1)
            seen = seen + pltpu.roll(seen, 32, 1)
            fluxes.append(seen - slot[p])
        fsend[it] = jnp.where(group % 2 == 0, fluxes[0], fluxes[1])
        fbuf[it, me] = fsend[it]

        @pl.loop(1, blocks)
        def _(d):
            remote(
                fsend.at[it], fbuf.at[it, me], phase_send.at[2 + it], phase_recv.at[2 + it],
                block_id(block_peer(d)),
            ).start()

    def spread_flux(it):
        whole(fbuf.at[it, pl.ds(0, blocks - 1)], 2 + it).wait_recv()
        seen = fbuf[it].reshape(blocks * 8, 128).astype(BF16)
        dense = jnp.zeros((lead, 128), F32)
        for p in range(2):
            half = select[p * blocks * 8 : (p + 1) * blocks * 8, :]
            every = lax.dot_general(seen, half, TN, preferred_element_type=F32)
            dense += every[lead * p : lead * p + lead, :]
        fall[it, row] = dense.astype(BF16)

        @pl.loop(1, n_row)
        def _(d):
            remote(
                fall.at[it, row], fall.at[it, row], phase_send.at[4 + it], phase_recv.at[4 + it],
                {"row": row_peer(d)},
            ).start()

    def new_share(it, old):
        whole(fall.at[it, pl.ds(0, n_row - 1)], 4 + it).wait_recv()
        if it == 0:
            whole(strip.at[pl.ds(0, n_row - 1)], 6).wait_recv()
        update = jnp.zeros((lead, share), F32)
        for r in range(n_row):
            update += jnp.dot(fall[it, r], strip[r], preferred_element_type=F32)
        return old + RELAXATION * update

    right_side(0)
    first_sweep(0, factors[0])
    halo_start(0)
    send_panel(5, 4)
    sweep(0, factors[1], False)
    halo_start(1)
    send_panel(9, 4)
    sweep(1, factors[2], False)
    halo_start(2)
    send_panel(13, n_row)
    sweep(2, factors[3], False, middle)
    send_flux(0, middle)
    halo_start(3)
    spread_flux(0)
    state = new_share(0, density[:, own])
    osend[0] = state
    rbuf[row] = state.astype(BF16)

    @pl.loop(1, n_row)
    def _(d):
        remote(
            rbuf.at[row], rbuf.at[row], phase_send.at[7], phase_recv.at[7], {"row": row_peer(d)}
        ).start()

    whole(rbuf.at[pl.ds(0, n_row - 1)], 7).wait_recv()

    send_potential(1, lambda k: rbuf[k])
    right_side(1)
    sweep(3, factors[0], False)
    halo_start(4)
    sweep(4, factors[1], False)
    halo_start(5)
    sweep(5, factors[2], False)
    halo_start(6)
    sweep(6, factors[3], True, inner)
    send_flux(1, inner)

    @pl.loop(0, 16, unroll=TURN)
    def _(i):
        x, y = i // 2, (i % 2) * 4
        tiles = quarters([inner[x, y + q] for q in range(4)])
        back = jnp.transpose(jnp.concatenate(tiles, axis=0))
        for q in range(4):
            volume_out[pl.ds(x * 8 + y + q, lead, stride=64), :] = back[lead * q : lead * q + lead, :]

    spread_flux(1)
    state = new_share(1, osend[0])
    osend[1] = state
    density_out[:, own] = state

    @pl.loop(1, n_row)
    def _(d):
        remote(
            osend.at[1], density_out.at[:, own], phase_send.at[8], phase_recv.at[8],
            {"row": row_peer(d)},
        ).start()

    whole(density_out.at[:, pl.ds(0, (n_row - 1) * share)], 8).wait_recv()

    for it in range(OUTER):
        whole(pbuf.at[it, pl.ds(0, blocks - 1)], it).wait_send()
        whole(fbuf.at[it, pl.ds(0, blocks - 1)], 2 + it).wait_send()
        whole(fall.at[it, pl.ds(0, n_row - 1)], 4 + it).wait_send()
    whole(strip.at[pl.ds(0, n_row - 1)], 6).wait_send()
    whole(rbuf.at[pl.ds(0, n_row - 1)], 7).wait_send()
    whole(density_out.at[:, pl.ds(0, (n_row - 1) * share)], 8).wait_send()
    for k in range(exchanges):
        halo_sent(k)


def local(panel, density, source, class_index, class_values, trace_count, trace_cell):
    sizes = (lax.axis_size("row"), lax.axis_size("col"), lax.axis_size("vol"))
    n_row, n_col, n_vol = sizes
    blocks = n_col * n_vol
    lead = source.shape[0]
    targets, nodes = panel.shape
    share = nodes // n_row
    ex = SWEEPS * OUTER - 1
    vmem = lambda shape, kind=F32: pltpu.VMEM(shape, kind)
    dma = pltpu.SemaphoreType.DMA
    density_out, volume = pl.pallas_call(
        functools.partial(kernel, sizes),
        out_shape=(
            jax.ShapeDtypeStruct(density.shape, F32),
            jax.ShapeDtypeStruct((lead * 64, 128), F32),
        ),
        in_specs=[pl.BlockSpec(memory_space=pltpu.VMEM)] * 4
        + [pl.BlockSpec(memory_space=pltpu.SMEM)] * 3,
        out_specs=(pl.BlockSpec(memory_space=pltpu.VMEM),) * 2,
        scratch_shapes=[
            vmem((blocks * SLOTS, targets), BF16),
            vmem((2048, 128), BF16),
            vmem((8, 8, 32, 128)),
            vmem((8, 8, 32, 128)),
            vmem((8, 8, 32, 128)),
            vmem((8, 8, 32, 128)),
            vmem((8, 8, 32, 128)),
            vmem((ex, 10, 10, 32, 128)),
            vmem((ex, 2, 2, 8, 128)),
            vmem((ex, 2, 8, 128)),
            vmem((ex, 2, 8, 128)),
            vmem((ex, 2, 8, 8, 128)),
            vmem((2, 8, 8, 128)),
            vmem((64, 128)),
            vmem((2, 8, 128)),
            vmem((SLOTS, 128)),
            vmem((OUTER, blocks, 8, 128)),
            vmem((OUTER, blocks, 8, 128)),
            vmem((OUTER, 8, 128)),
            vmem((OUTER, blocks, 8, 128)),
            vmem((OUTER, n_row, lead, targets), BF16),
            vmem((n_row, targets, share), BF16),
            vmem((n_row, lead, share), BF16),
            vmem((OUTER, lead, share)),
            dma((ex, 6)),
            dma((ex, 6)),
            dma((9,)),
            dma((9,)),
        ],
        compiler_params=pltpu.CompilerParams(
            collective_id=0, has_side_effects=True, vmem_limit_bytes=56 * 1024 * 1024
        ),
    )(
        panel,
        density,
        source.reshape(lead * 64, 128),
        class_index.reshape(64, 128),
        class_values,
        trace_count,
        trace_cell,
    )
    return density_out, volume.reshape(source.shape)


def solution(mesh):
    placed = (
        P("row", ("col", "vol")),
        P(None, ("col", "vol")),
        P(None, "row", "col", "vol"),
        P("row", "col", "vol"),
        P(),
        P("row", None),
        P("row", None, None),
    )
    return jax.shard_map(
        local,
        mesh=mesh,
        in_specs=placed,
        out_specs=(P(None, ("col", "vol")), P(None, "row", "col", "vol")),
        check_vma=False,
    )
```

```python
import functools
import math

import jax
import jax.numpy as jnp
from jax import lax
from jax.experimental import pallas as pl
from jax.experimental.pallas import tpu as pltpu
from jax.sharding import PartitionSpec as P

SWEEPS = 4
OUTER = 2
MASS_TERM = 0.1
RELAXATION = 0.5
SPECTRUM_LOW = 0.1
SPECTRUM_HIGH = 2.0
MESH = pl.DeviceIdType.MESH
F32 = jnp.float32
BF16 = jnp.bfloat16
NT = (((1,), (1,)), ((), ()))
TN = (((0,), (0,)), ((), ()))
SLOTS = 16
TURN = 4
SPANS = tuple(slice(8 * b, 8 * b + 8) for b in range(4))


def relax_factors(count):
    middle = (SPECTRUM_HIGH + SPECTRUM_LOW) / 2.0
    spread = (SPECTRUM_HIGH - SPECTRUM_LOW) / 2.0
    return [
        1.0 / (middle + spread * math.cos(math.pi * (2 * order + 1) / (2 * count)))
        for order in range(count)
    ]


def kernel(
    sizes,
    panel, density, source, class_index, class_values, trace_count, trace_cell,
    density_out, volume_out,
    select, hits, conduct, inverse, inner, middle, base, field, zface, zlo, zhi, zrow, zmix,
    turned, slot, picked, psend, pbuf, fsend, fbuf, fall, strip, rbuf, osend,
    halo_send, halo_recv, phase_send, phase_recv, gather_send, gather_recv,
):
    n_row, n_col, n_vol = sizes
    blocks = n_col * n_vol
    share = density.shape[1] // n_row
    lead = density.shape[0]
    factors = relax_factors(SWEEPS)
    row = lax.axis_index("row")
    col = lax.axis_index("col")
    vol = lax.axis_index("vol")
    me = col * n_vol + vol

    def block_id(j):
        return {"col": j // n_vol, "vol": j % n_vol}

    def block_peer(d):
        return lax.rem(me + d, blocks)

    def row_peer(d):
        return lax.rem(row + d, n_row)

    barrier = pltpu.get_barrier_semaphore()

    @pl.loop(1, blocks)
    def _(d):
        pl.semaphore_signal(barrier, inc=1, device_id=block_id(block_peer(d)), device_id_type=MESH)

    @pl.loop(1, n_row)
    def _(d):
        pl.semaphore_signal(barrier, inc=1, device_id={"row": row_peer(d)}, device_id_type=MESH)

    def remote(src, dst, send, recv, device):
        return pltpu.make_async_remote_copy(
            src_ref=src, dst_ref=dst, send_sem=send, recv_sem=recv,
            device_id=device, device_id_type=MESH,
        )

    def whole(ref, phase):
        return remote(ref, ref, phase_send.at[phase], phase_recv.at[phase], {"row": row})

    sub = lax.broadcasted_iota(jnp.int32, (8, 128), 0)
    lane = lax.broadcasted_iota(jnp.int32, (8, 128), 1)
    group = lane // 32
    exchanges = field.shape[0]

    def pieces(x):
        first = x.astype(BF16)
        rest = x - first.astype(F32)
        second = rest.astype(BF16)
        third = (rest - second.astype(F32)).astype(BF16)
        return first, second, third

    offset = jnp.int32(0)
    marks = []
    for j in range(blocks):
        count = trace_count[0, j]
        marks.append((offset, count))
        offset = offset + count
    for p in range(2):
        for j in range(0, blocks, 2):
            both = []
            for start, count in marks[j : j + 2]:
                s = sub + 8 * p
                both.append(jnp.where((lane == s + start) & (s < count), 1.0, 0.0).astype(F32))
            at = p * blocks * 8 + j * 8
            select[at : at + 16, :] = jnp.concatenate(both, axis=0).astype(BF16)

    def quarters(tiles):
        a = list(tiles)
        grp = lax.broadcasted_iota(jnp.int32, a[0].shape, 1) // 32
        for step in (2, 1):
            out = list(a)
            for i in range(4):
                if i & step == 0:
                    j = i | step
                    shift = 32 * step
                    keep = (grp & step) == 0
                    out[i] = jnp.where(keep, a[i], pltpu.roll(a[j], shift, 1))
                    out[j] = jnp.where(keep, pltpu.roll(a[i], 128 - shift, 1), a[j])
            a = out
        return a

    def to_inner(rows, write):
        @pl.loop(0, 16, unroll=TURN)
        def _(i):
            x, y = i // 2, (i % 2) * 4
            stacked = jnp.concatenate([rows(x, y + q) for q in range(4)], axis=0)
            flipped = jnp.transpose(stacked)
            for q, tile in enumerate(quarters([flipped[32 * q : 32 * q + 32, :] for q in range(4)])):
                write(x, y + q, tile)

    cls = class_index[...]
    value = jnp.zeros(cls.shape, F32)
    for k in range(class_values.shape[0]):
        value = jnp.where(cls == k, class_values[k], value)
    turned[...] = value

    def coefficients(x, y, tile):
        inv = 1.0 / (MASS_TERM + 6.0 * tile)
        inverse[x, y] = inv
        conduct[x, y] = tile * inv

    def prepare():
        to_inner(
            lambda x, y: jnp.broadcast_to(turned[pl.ds(x * 8 + y, 1), :], (lead, 128)), coefficients
        )

    def send_potential(it, chunk):
        partial = jnp.zeros((panel.shape[0], 128), F32)
        for k in range(n_row):
            part = chunk(k)
            partial += lax.dot_general(
                panel[:, k * share : (k + 1) * share],
                jnp.concatenate([part] * (128 // lead), axis=0),
                NT, preferred_element_type=F32,
            )
        chosen = jnp.zeros((select.shape[0], 128), F32)
        for piece in pieces(partial):
            chosen += jnp.dot(select[...], piece, preferred_element_type=F32)
        half = blocks * 8
        for j in range(blocks):
            psend[it, j] = jnp.where(
                group % 2 == 0, chosen[8 * j : 8 * j + 8, :],
                chosen[half + 8 * j : half + 8 * j + 8, :],
            )
        if it == 0:
            prepare()
            pl.semaphore_wait(barrier, blocks - 1 + n_row - 1)
        pbuf[it, me] = psend[it, me]

        @pl.loop(1, blocks)
        def _(d):
            j = block_peer(d)
            remote(
                psend.at[it, j], pbuf.at[it, me], phase_send.at[it], phase_recv.at[it], block_id(j)
            ).start()

    def panel_copy(d):
        r = row_peer(d)
        return remote(
            panel.at[:, pl.ds(pl.multiple_of(r * share, share), share)], strip.at[row],
            phase_send.at[6], phase_recv.at[6], {"row": r},
        )

    order = sorted(range(1, n_row), key=lambda d: -min(d, n_row - d))
    head = max(1, n_row // 4)
    rest = order[head:]
    rest = [d for pair in zip(rest, reversed(rest)) for d in pair][: len(rest)]
    batches = [order[:head]] + [rest[i::4] for i in range(4)]

    def send_panel(i):
        for d in batches[i]:
            panel_copy(d).start()

    near = min(4, n_row)
    far = n_row // near

    def gather(i, cut):
        def copy(r, peer):
            return remote(
                cut(r), cut(r), gather_send.at[i, r, peer], gather_recv.at[i, r], {"row": peer}
            )

        base_row = row - lax.rem(row, near)
        nears = [base_row + lax.rem(row + d, near) for d in range(1, near)]
        fars = [lax.rem(row + near * d, n_row) for d in range(1, far)]
        for peer in fars + nears:
            copy(row, peer).start()
        for r in fars:
            copy(r, row).wait_recv()
            for peer in nears:
                copy(r, peer).start()
        for peer in nears:
            for q in range(far):
                copy(lax.rem(peer + near * q, n_row), row).wait_recv()

        def sent():
            for peer in fars + nears:
                copy(row, peer).wait_send()
            for r in fars:
                for peer in nears:
                    copy(r, peer).wait_send()

        return sent

    own = pl.ds(pl.multiple_of(row * share, share), share)
    send_potential(0, lambda k: density[:, k * share : (k + 1) * share].astype(BF16))
    strip[row] = panel[:, own]
    send_panel(0)

    own_count = trace_count[0, me]
    cells, spot = [], jnp.full((8, 128), -1, jnp.int32)
    quarter = [jnp.full((8, 128), -1, jnp.int32) for _ in range(2)]
    for s in range(SLOTS):
        cell = jnp.where(s < own_count, trace_cell[0, me, s], -1)
        place = (cell >> 7) * 32 + (cell & 31)
        spot = jnp.where(lane % SLOTS == s, jnp.where(cell >= 0, place, -1), spot)
        fourth = jnp.where(cell >= 0, (cell >> 5) & 3, -1)
        quarter[s // 8] = jnp.where(sub == s % 8, fourth, quarter[s // 8])
        cells.append(jnp.maximum(place, 0))
    mine = [jnp.where(quarter[p] == group, 1.0, 0.0).astype(F32) for p in range(2)]
    spot = jnp.where(lane < 3 * SLOTS, spot, -1)

    @pl.loop(0, 128)
    def _(i):
        at = pl.multiple_of(i * 16, 16)
        here = jnp.concatenate([sub, sub + 8], axis=0) + at
        wide = jnp.concatenate([spot, spot], axis=0)
        hits[pl.ds(at, 16), :] = jnp.where(here == wide, 1.0, 0.0).astype(BF16)

    def keep_source(x, y, tile):
        inner[x, y] = tile

    to_inner(lambda x, y: source[pl.ds(x * 8 + y, lead, stride=64), :], keep_source)

    def clear(write):
        @pl.loop(0, exchanges)
        def _(k):
            write(k)

    def clear_x(k, x):
        field[k, x] = jnp.zeros(field.shape[2:], F32)

    def clear_y(k, y):
        @pl.loop(0, 10)
        def _(x):
            field[k, x, y] = jnp.zeros(field.shape[3:], F32)

    def clear_z(ref, k):
        ref[k] = jnp.zeros(ref.shape[1:], F32)

    for here, edge, write in (
        (row, 0, lambda k: clear_x(k, 0)), (row, n_row - 1, lambda k: clear_x(k, 9)),
        (col, 0, lambda k: clear_y(k, 0)), (col, n_col - 1, lambda k: clear_y(k, 9)),
        (vol, 0, lambda k: clear_z(zlo, k)), (vol, n_vol - 1, lambda k: clear_z(zhi, k)),
    ):
        @pl.when(here == edge)
        def _(write=write):
            clear(write)

    def right_side(it):
        whole(pbuf.at[it, pl.ds(0, blocks - 1)], it).wait_recv()
        total = pbuf[it, 0]
        for j in range(1, blocks):
            total += pbuf[it, j]
        swapped = pltpu.roll(total, 32, 1)
        even = group % 2 == 0
        parts = [jnp.where(even, total, swapped), jnp.where(even, swapped, total)]
        for p in range(2):
            slot[p] = parts[p]
        placed = jnp.concatenate([parts[p] * mine[p] for p in range(2)], axis=0)
        values = jnp.concatenate(
            list(pieces(placed)) + [jnp.zeros((128 - 3 * SLOTS, 128), BF16)], axis=0
        )

        @pl.loop(0, 8)
        def _(x):
            at = pl.multiple_of(x * 256, 256)
            added = jnp.dot(hits[pl.ds(at, 256), :], values, preferred_element_type=F32)
            for y in range(8):
                base[x, y] = (inner[x, y] + added[32 * y : 32 * y + 32, :]) * inverse[x, y]

    def keep(k, x, y, new, packed):
        low, top = packed
        for b in range(4):
            field[k, x + 1, y + 1, SPANS[b], :] = new[b]
        low = jnp.where(sub == y, pltpu.roll(new[0], y, 0) if y else new[0], low)
        top = jnp.where(sub == y, pltpu.roll(new[3], y + 1, 0) if y < 7 else new[3], top)
        return low, top

    def pack_rows(k):
        for side, edge in ((0, 0), (1, 3)):
            for b in range(2):
                packed = jnp.zeros((8, 128), F32)
                for i in range(4):
                    moved = zrow[k, side, 4 * b + i]
                    if i != edge:
                        moved = pltpu.roll(moved, (32 * (i - edge)) % 128, 1)
                    packed = jnp.where(group == i, moved, packed)
                zface[k, side, b] = packed

    def first_sweep(k, factor):
        @pl.loop(0, 8)
        def _(x):
            packed = (jnp.zeros((8, 128), F32),) * 2
            for y in range(8):
                new = [factor * base[x, y, SPANS[b], :] for b in range(4)]
                packed = keep(k, x, y, new, packed)
            zrow[k, 0, x], zrow[k, 1, x] = packed

        pack_rows(k)

    def halo_copies(k):
        pairs = (
            (row < n_row - 1, field.at[k, 8, pl.ds(1, 8)], field.at[k, 0, pl.ds(1, 8)], {"row": row + 1}),
            (row > 0, field.at[k, 1, pl.ds(1, 8)], field.at[k, 9, pl.ds(1, 8)], {"row": row - 1}),
            (col < n_col - 1, field.at[k, pl.ds(1, 8), 8], field.at[k, pl.ds(1, 8), 0], {"col": col + 1}),
            (col > 0, field.at[k, pl.ds(1, 8), 1], field.at[k, pl.ds(1, 8), 9], {"col": col - 1}),
            (vol < n_vol - 1, zface.at[k, 1], zlo.at[k], {"vol": vol + 1}),
            (vol > 0, zface.at[k, 0], zhi.at[k], {"vol": vol - 1}),
        )
        return [
            (go, remote(src, dst, halo_send.at[k, i], halo_recv.at[k, i], device))
            for i, (go, src, dst, device) in enumerate(pairs)
        ]

    arrives = (row > 0, row < n_row - 1, col > 0, col < n_col - 1, vol > 0, vol < n_vol - 1)

    def halo_start(k):
        copies = halo_copies(k)
        for i in (4, 5, 0, 1, 2, 3):
            @pl.when(copies[i][0])
            def _(copy=copies[i][1]):
                copy.start()

    def halo_wait(k):
        for i, (_, copy) in enumerate(halo_copies(k)):
            @pl.when(arrives[i])
            def _(copy=copy):
                copy.wait_recv()

    def halo_sent(k):
        for go, copy in halo_copies(k):
            @pl.when(go)
            def _(copy=copy):
                copy.wait_send()

    def sweep(k, factor, last, seen=None):
        halo_wait(k)
        for x in range(8):
            b, i = x // 4, x % 4
            low, top = zlo[k, b], zhi[k, b]
            low = pltpu.roll(low, 32 * (3 - i), 1) if i < 3 else low
            top = pltpu.roll(top, (128 - 32 * i) % 128, 1) if i else top
            zmix[0, x] = pltpu.roll(jnp.where(group == 3, low, zrow[k, 1, x]), 32, 1)
            zmix[1, x] = pltpu.roll(jnp.where(group == 0, top, zrow[k, 0, x]), 96, 1)

        @pl.loop(0, 8)
        def _(x):
            packed = (jnp.zeros((8, 128), F32),) * 2
            for y in range(8):
                c = [field[k, x + 1, y + 1, SPANS[b], :] for b in range(4)]
                ups = [pltpu.roll(v, 1, 0) for v in c]
                downs = [pltpu.roll(v, 7, 0) for v in c]
                new = []
                for b in range(4):
                    before = zmix[0, x, y : y + 1, :] if b == 0 else ups[b - 1]
                    after = zmix[1, x, y : y + 1, :] if b == 3 else downs[b + 1]
                    up = jnp.where(sub == 0, before, ups[b])
                    down = jnp.where(sub == 7, after, downs[b])
                    sp = SPANS[b]
                    around = (
                        (field[k, x, y + 1, sp, :] + field[k, x + 2, y + 1, sp, :])
                        + (field[k, x + 1, y, sp, :] + field[k, x + 1, y + 2, sp, :])
                        + (up + down)
                    )
                    new.append(
                        (1.0 - factor) * c[b]
                        + factor * (base[x, y, sp, :] + conduct[x, y, sp, :] * around)
                    )
                if seen is not None:
                    for b in range(4):
                        seen[x, y, SPANS[b], :] = new[b]
                if not last:
                    packed = keep(k + 1, x, y, new, packed)
            if not last:
                zrow[k + 1, 0, x], zrow[k + 1, 1, x] = packed

        if not last:
            pack_rows(k + 1)

    def send_flux(it, ref):
        for s in range(SLOTS):
            place = cells[s]
            picked[s : s + 1, :] = ref[
                place >> 8, (place >> 5) & 7, pl.ds(place & 31, 1), :
            ]
        fluxes = []
        for p in range(2):
            seen = picked[8 * p : 8 * p + 8, :] * mine[p]
            seen = seen + pltpu.roll(seen, 64, 1)
            seen = seen + pltpu.roll(seen, 32, 1)
            fluxes.append(seen - slot[p])
        fsend[it] = jnp.where(group % 2 == 0, fluxes[0], fluxes[1])
        fbuf[it, me] = fsend[it]

        @pl.loop(1, blocks)
        def _(d):
            remote(
                fsend.at[it], fbuf.at[it, me], phase_send.at[2 + it], phase_recv.at[2 + it],
                block_id(block_peer(d)),
            ).start()

    def spread_flux(it):
        whole(fbuf.at[it, pl.ds(0, blocks - 1)], 2 + it).wait_recv()
        seen = fbuf[it].reshape(blocks * 8, 128).astype(BF16)
        dense = jnp.zeros((lead, 128), F32)
        for p in range(2):
            half = select[p * blocks * 8 : (p + 1) * blocks * 8, :]
            every = lax.dot_general(seen, half, TN, preferred_element_type=F32)
            dense += every[lead * p : lead * p + lead, :]
        fall[it, row] = dense.astype(BF16)

        @pl.loop(1, n_row)
        def _(d):
            remote(
                fall.at[it, row], fall.at[it, row], phase_send.at[4 + it], phase_recv.at[4 + it],
                {"row": row_peer(d)},
            ).start()

    def new_share(it, old):
        whole(fall.at[it, pl.ds(0, n_row - 1)], 4 + it).wait_recv()
        if it == 0:
            whole(strip.at[pl.ds(0, n_row - 1)], 6).wait_recv()
        update = jnp.zeros((lead, share), F32)
        for r in range(n_row):
            update += jnp.dot(fall[it, r], strip[r], preferred_element_type=F32)
        return old + RELAXATION * update

    right_side(0)
    first_sweep(0, factors[0])
    halo_start(0)
    send_panel(1)
    sweep(0, factors[1], False)
    halo_start(1)
    send_panel(2)
    sweep(1, factors[2], False)
    halo_start(2)
    send_panel(3)
    sweep(2, factors[3], False, middle)
    send_flux(0, middle)
    halo_start(3)
    send_panel(4)
    spread_flux(0)
    state = new_share(0, density[:, own])
    osend[0] = state
    rbuf[row] = state.astype(BF16)

    sent_rounded = gather(0, lambda r: rbuf.at[r])

    send_potential(1, lambda k: rbuf[k])
    right_side(1)
    sweep(3, factors[0], False)
    halo_start(4)
    sweep(4, factors[1], False)
    halo_start(5)
    sweep(5, factors[2], False)
    halo_start(6)
    sweep(6, factors[3], True, inner)
    send_flux(1, inner)

    @pl.loop(0, 16, unroll=TURN)
    def _(i):
        x, y = i // 2, (i % 2) * 4
        tiles = quarters([inner[x, y + q] for q in range(4)])
        back = jnp.transpose(jnp.concatenate(tiles, axis=0))
        for q in range(4):
            volume_out[pl.ds(x * 8 + y + q, lead, stride=64), :] = back[lead * q : lead * q + lead, :]

    spread_flux(1)
    state = new_share(1, osend[0])
    density_out[:, own] = state

    sent_final = gather(
        1, lambda r: density_out.at[:, pl.ds(pl.multiple_of(r * share, share), share)]
    )

    for it in range(OUTER):
        whole(pbuf.at[it, pl.ds(0, blocks - 1)], it).wait_send()
        whole(fbuf.at[it, pl.ds(0, blocks - 1)], 2 + it).wait_send()
        whole(fall.at[it, pl.ds(0, n_row - 1)], 4 + it).wait_send()
    whole(strip.at[pl.ds(0, n_row - 1)], 6).wait_send()
    sent_rounded()
    sent_final()
    for k in range(exchanges):
        halo_sent(k)


def local(panel, density, source, class_index, class_values, trace_count, trace_cell):
    sizes = (lax.axis_size("row"), lax.axis_size("col"), lax.axis_size("vol"))
    n_row, n_col, n_vol = sizes
    blocks = n_col * n_vol
    lead = source.shape[0]
    targets, nodes = panel.shape
    share = nodes // n_row
    ex = SWEEPS * OUTER - 1
    vmem = lambda shape, kind=F32: pltpu.VMEM(shape, kind)
    dma = pltpu.SemaphoreType.DMA
    density_out, volume = pl.pallas_call(
        functools.partial(kernel, sizes),
        out_shape=(
            jax.ShapeDtypeStruct(density.shape, F32),
            jax.ShapeDtypeStruct((lead * 64, 128), F32),
        ),
        in_specs=[pl.BlockSpec(memory_space=pltpu.VMEM)] * 4
        + [pl.BlockSpec(memory_space=pltpu.SMEM)] * 3,
        out_specs=(pl.BlockSpec(memory_space=pltpu.VMEM),) * 2,
        scratch_shapes=[
            vmem((blocks * SLOTS, targets), BF16),
            vmem((2048, 128), BF16),
            vmem((8, 8, 32, 128)),
            vmem((8, 8, 32, 128)),
            vmem((8, 8, 32, 128)),
            vmem((8, 8, 32, 128)),
            vmem((8, 8, 32, 128)),
            vmem((ex, 10, 10, 32, 128)),
            vmem((ex, 2, 2, 8, 128)),
            vmem((ex, 2, 8, 128)),
            vmem((ex, 2, 8, 128)),
            vmem((ex, 2, 8, 8, 128)),
            vmem((2, 8, 8, 128)),
            vmem((64, 128)),
            vmem((2, 8, 128)),
            vmem((SLOTS, 128)),
            vmem((OUTER, blocks, 8, 128)),
            vmem((OUTER, blocks, 8, 128)),
            vmem((OUTER, 8, 128)),
            vmem((OUTER, blocks, 8, 128)),
            vmem((OUTER, n_row, lead, targets), BF16),
            vmem((n_row, targets, share), BF16),
            vmem((n_row, lead, share), BF16),
            vmem((1, lead, share)),
            dma((ex, 6)),
            dma((ex, 6)),
            dma((7,)),
            dma((7,)),
            dma((2, n_row, n_row)),
            dma((2, n_row)),
        ],
        compiler_params=pltpu.CompilerParams(
            collective_id=0, has_side_effects=True, vmem_limit_bytes=56 * 1024 * 1024
        ),
    )(
        panel,
        density,
        source.reshape(lead * 64, 128),
        class_index.reshape(64, 128),
        class_values,
        trace_count,
        trace_cell,
    )
    return density_out, volume.reshape(source.shape)


def solution(mesh):
    placed = (
        P("row", ("col", "vol")),
        P(None, ("col", "vol")),
        P(None, "row", "col", "vol"),
        P("row", "col", "vol"),
        P(),
        P("row", None),
        P("row", None, None),
    )
    return jax.shard_map(
        local,
        mesh=mesh,
        in_specs=placed,
        out_specs=(P(None, ("col", "vol")), P(None, "row", "col", "vol")),
        check_vma=False,
    )
```

```python
import functools
import math

import jax
import jax.numpy as jnp
from jax import lax
from jax.experimental import pallas as pl
from jax.experimental.pallas import tpu as pltpu
from jax.sharding import PartitionSpec as P

SWEEPS = 4
OUTER = 2
MASS_TERM = 0.1
RELAXATION = 0.5
SPECTRUM_LOW = 0.1
SPECTRUM_HIGH = 2.0
MESH = pl.DeviceIdType.MESH
F32 = jnp.float32
BF16 = jnp.bfloat16
NT = (((1,), (1,)), ((), ()))
TN = (((0,), (0,)), ((), ()))
SLOTS = 16
TURN = 4
SPANS = tuple(slice(8 * b, 8 * b + 8) for b in range(4))


def relax_factors(count):
    middle = (SPECTRUM_HIGH + SPECTRUM_LOW) / 2.0
    spread = (SPECTRUM_HIGH - SPECTRUM_LOW) / 2.0
    return [
        1.0 / (middle + spread * math.cos(math.pi * (2 * order + 1) / (2 * count)))
        for order in range(count)
    ]


def kernel(
    sizes,
    panel, density, source, class_index, class_values, trace_count, trace_cell,
    density_out, volume_out,
    select, hits, conduct, inverse, inner, middle, base, field, zface, zlo, zhi, zrow, zmix,
    turned, slot, picked, psend, pbuf, fsend, fbuf, fall, strip, usend, urecv, rbuf, osend,
    halo_send, halo_recv, phase_send, phase_recv, gather_send, gather_recv,
):
    n_row, n_col, n_vol = sizes
    blocks = n_col * n_vol
    share = density.shape[1] // n_row
    lead = density.shape[0]
    factors = relax_factors(SWEEPS)
    row = lax.axis_index("row")
    col = lax.axis_index("col")
    vol = lax.axis_index("vol")
    me = col * n_vol + vol

    def block_id(j):
        return {"col": j // n_vol, "vol": j % n_vol}

    def block_peer(d):
        return lax.rem(me + d, blocks)

    def row_peer(d):
        return lax.rem(row + d, n_row)

    barrier = pltpu.get_barrier_semaphore()

    @pl.loop(1, blocks)
    def _(d):
        pl.semaphore_signal(barrier, inc=1, device_id=block_id(block_peer(d)), device_id_type=MESH)

    @pl.loop(1, n_row)
    def _(d):
        pl.semaphore_signal(barrier, inc=1, device_id={"row": row_peer(d)}, device_id_type=MESH)

    def remote(src, dst, send, recv, device):
        return pltpu.make_async_remote_copy(
            src_ref=src, dst_ref=dst, send_sem=send, recv_sem=recv,
            device_id=device, device_id_type=MESH,
        )

    def whole(ref, phase):
        return remote(ref, ref, phase_send.at[phase], phase_recv.at[phase], {"row": row})

    sub = lax.broadcasted_iota(jnp.int32, (8, 128), 0)
    lane = lax.broadcasted_iota(jnp.int32, (8, 128), 1)
    group = lane // 32
    exchanges = field.shape[0]

    def pieces(x):
        first = x.astype(BF16)
        rest = x - first.astype(F32)
        second = rest.astype(BF16)
        third = (rest - second.astype(F32)).astype(BF16)
        return first, second, third

    offset = jnp.int32(0)
    marks = []
    for j in range(blocks):
        count = trace_count[0, j]
        marks.append((offset, count))
        offset = offset + count
    for p in range(2):
        for j in range(0, blocks, 2):
            both = []
            for start, count in marks[j : j + 2]:
                s = sub + 8 * p
                both.append(jnp.where((lane == s + start) & (s < count), 1.0, 0.0).astype(F32))
            at = p * blocks * 8 + j * 8
            select[at : at + 16, :] = jnp.concatenate(both, axis=0).astype(BF16)

    def quarters(tiles):
        a = list(tiles)
        grp = lax.broadcasted_iota(jnp.int32, a[0].shape, 1) // 32
        for step in (2, 1):
            out = list(a)
            for i in range(4):
                if i & step == 0:
                    j = i | step
                    shift = 32 * step
                    keep = (grp & step) == 0
                    out[i] = jnp.where(keep, a[i], pltpu.roll(a[j], shift, 1))
                    out[j] = jnp.where(keep, pltpu.roll(a[i], 128 - shift, 1), a[j])
            a = out
        return a

    def to_inner(rows, write):
        @pl.loop(0, 16, unroll=TURN)
        def _(i):
            x, y = i // 2, (i % 2) * 4
            stacked = jnp.concatenate([rows(x, y + q) for q in range(4)], axis=0)
            flipped = jnp.transpose(stacked)
            for q, tile in enumerate(quarters([flipped[32 * q : 32 * q + 32, :] for q in range(4)])):
                write(x, y + q, tile)

    cls = class_index[...]
    value = jnp.zeros(cls.shape, F32)
    for k in range(class_values.shape[0]):
        value = jnp.where(cls == k, class_values[k], value)
    turned[...] = value

    def coefficients(x, y, tile):
        inv = 1.0 / (MASS_TERM + 6.0 * tile)
        inverse[x, y] = inv
        conduct[x, y] = tile * inv

    def prepare():
        to_inner(
            lambda x, y: jnp.broadcast_to(turned[pl.ds(x * 8 + y, 1), :], (lead, 128)), coefficients
        )

    def send_potential(it, chunk):
        partial = jnp.zeros((panel.shape[0], 128), F32)
        for k in range(n_row):
            part = chunk(k)
            partial += lax.dot_general(
                panel[:, k * share : (k + 1) * share],
                jnp.concatenate([part] * (128 // lead), axis=0),
                NT, preferred_element_type=F32,
            )
        chosen = jnp.zeros((select.shape[0], 128), F32)
        for piece in pieces(partial):
            chosen += jnp.dot(select[...], piece, preferred_element_type=F32)
        half = blocks * 8
        for j in range(blocks):
            psend[it, j] = jnp.where(
                group % 2 == 0, chosen[8 * j : 8 * j + 8, :],
                chosen[half + 8 * j : half + 8 * j + 8, :],
            )
        if it == 0:
            prepare()
            pl.semaphore_wait(barrier, blocks - 1 + n_row - 1)
        pbuf[it, me] = psend[it, me]

        @pl.loop(1, blocks)
        def _(d):
            j = block_peer(d)
            remote(
                psend.at[it, j], pbuf.at[it, me], phase_send.at[it], phase_recv.at[it], block_id(j)
            ).start()

    near = min(4, n_row)
    far = n_row // near

    base_row = row - lax.rem(row, near)
    mine_near = lax.rem(row, near)
    mine_far = row // near
    nears = [base_row + lax.rem(row + d, near) for d in range(1, near)]
    fars = [lax.rem(row + near * d, n_row) for d in range(1, far)]

    def panel_copy(d, f):
        r = base_row + lax.rem(row + d, near)
        at = (near * f + lax.rem(r, near)) * share
        return remote(
            panel.at[:, pl.ds(pl.multiple_of(at, share), share)], strip.at[mine_near, f],
            phase_send.at[6], phase_recv.at[6], {"row": r},
        )

    chunks = [(d, f) for f in range(far) for d in range(1, near)]
    per = (len(chunks) + 3) // 4

    def send_panel(i):
        for d, f in chunks[i * per : (i + 1) * per]:
            panel_copy(d, f).start()

    def gather(i, cut):
        def copy(r, peer):
            return remote(
                cut(r), cut(r), gather_send.at[i, r, peer], gather_recv.at[i, r], {"row": peer}
            )

        for peer in fars + nears:
            copy(row, peer).start()
        for r in fars:
            copy(r, row).wait_recv()
            for peer in nears:
                copy(r, peer).start()
        for peer in nears:
            for q in range(far):
                copy(lax.rem(peer + near * q, n_row), row).wait_recv()

        def sent():
            for peer in fars + nears:
                copy(row, peer).wait_send()
            for r in fars:
                for peer in nears:
                    copy(r, peer).wait_send()

        return sent

    own = pl.ds(pl.multiple_of(row * share, share), share)
    send_potential(0, lambda k: density[:, k * share : (k + 1) * share].astype(BF16))
    for f in range(far):
        at = (near * f + mine_near) * share
        strip[mine_near, f] = panel[:, pl.ds(pl.multiple_of(at, share), share)]
    send_panel(0)

    own_count = trace_count[0, me]
    cells, spot = [], jnp.full((8, 128), -1, jnp.int32)
    quarter = [jnp.full((8, 128), -1, jnp.int32) for _ in range(2)]
    for s in range(SLOTS):
        cell = jnp.where(s < own_count, trace_cell[0, me, s], -1)
        place = (cell >> 7) * 32 + (cell & 31)
        spot = jnp.where(lane % SLOTS == s, jnp.where(cell >= 0, place, -1), spot)
        fourth = jnp.where(cell >= 0, (cell >> 5) & 3, -1)
        quarter[s // 8] = jnp.where(sub == s % 8, fourth, quarter[s // 8])
        cells.append(jnp.maximum(place, 0))
    mine = [jnp.where(quarter[p] == group, 1.0, 0.0).astype(F32) for p in range(2)]
    spot = jnp.where(lane < 3 * SLOTS, spot, -1)

    @pl.loop(0, 128)
    def _(i):
        at = pl.multiple_of(i * 16, 16)
        here = jnp.concatenate([sub, sub + 8], axis=0) + at
        wide = jnp.concatenate([spot, spot], axis=0)
        hits[pl.ds(at, 16), :] = jnp.where(here == wide, 1.0, 0.0).astype(BF16)

    def keep_source(x, y, tile):
        inner[x, y] = tile

    to_inner(lambda x, y: source[pl.ds(x * 8 + y, lead, stride=64), :], keep_source)

    def clear(write):
        @pl.loop(0, exchanges)
        def _(k):
            write(k)

    def clear_x(k, x):
        field[k, x] = jnp.zeros(field.shape[2:], F32)

    def clear_y(k, y):
        @pl.loop(0, 10)
        def _(x):
            field[k, x, y] = jnp.zeros(field.shape[3:], F32)

    def clear_z(ref, k):
        ref[k] = jnp.zeros(ref.shape[1:], F32)

    for here, edge, write in (
        (row, 0, lambda k: clear_x(k, 0)), (row, n_row - 1, lambda k: clear_x(k, 9)),
        (col, 0, lambda k: clear_y(k, 0)), (col, n_col - 1, lambda k: clear_y(k, 9)),
        (vol, 0, lambda k: clear_z(zlo, k)), (vol, n_vol - 1, lambda k: clear_z(zhi, k)),
    ):
        @pl.when(here == edge)
        def _(write=write):
            clear(write)

    def right_side(it):
        whole(pbuf.at[it, pl.ds(0, blocks - 1)], it).wait_recv()
        total = pbuf[it, 0]
        for j in range(1, blocks):
            total += pbuf[it, j]
        swapped = pltpu.roll(total, 32, 1)
        even = group % 2 == 0
        parts = [jnp.where(even, total, swapped), jnp.where(even, swapped, total)]
        for p in range(2):
            slot[p] = parts[p]
        placed = jnp.concatenate([parts[p] * mine[p] for p in range(2)], axis=0)
        values = jnp.concatenate(
            list(pieces(placed)) + [jnp.zeros((128 - 3 * SLOTS, 128), BF16)], axis=0
        )

        @pl.loop(0, 8)
        def _(x):
            at = pl.multiple_of(x * 256, 256)
            added = jnp.dot(hits[pl.ds(at, 256), :], values, preferred_element_type=F32)
            for y in range(8):
                base[x, y] = (inner[x, y] + added[32 * y : 32 * y + 32, :]) * inverse[x, y]

    def keep(k, x, y, new, packed):
        low, top = packed
        for b in range(4):
            field[k, x + 1, y + 1, SPANS[b], :] = new[b]
        low = jnp.where(sub == y, pltpu.roll(new[0], y, 0) if y else new[0], low)
        top = jnp.where(sub == y, pltpu.roll(new[3], y + 1, 0) if y < 7 else new[3], top)
        return low, top

    def pack_rows(k):
        for side, edge in ((0, 0), (1, 3)):
            for b in range(2):
                packed = jnp.zeros((8, 128), F32)
                for i in range(4):
                    moved = zrow[k, side, 4 * b + i]
                    if i != edge:
                        moved = pltpu.roll(moved, (32 * (i - edge)) % 128, 1)
                    packed = jnp.where(group == i, moved, packed)
                zface[k, side, b] = packed

    def first_sweep(k, factor):
        @pl.loop(0, 8)
        def _(x):
            packed = (jnp.zeros((8, 128), F32),) * 2
            for y in range(8):
                new = [factor * base[x, y, SPANS[b], :] for b in range(4)]
                packed = keep(k, x, y, new, packed)
            zrow[k, 0, x], zrow[k, 1, x] = packed

        pack_rows(k)

    def halo_copies(k):
        pairs = (
            (row < n_row - 1, field.at[k, 8, pl.ds(1, 8)], field.at[k, 0, pl.ds(1, 8)], {"row": row + 1}),
            (row > 0, field.at[k, 1, pl.ds(1, 8)], field.at[k, 9, pl.ds(1, 8)], {"row": row - 1}),
            (col < n_col - 1, field.at[k, pl.ds(1, 8), 8], field.at[k, pl.ds(1, 8), 0], {"col": col + 1}),
            (col > 0, field.at[k, pl.ds(1, 8), 1], field.at[k, pl.ds(1, 8), 9], {"col": col - 1}),
            (vol < n_vol - 1, zface.at[k, 1], zlo.at[k], {"vol": vol + 1}),
            (vol > 0, zface.at[k, 0], zhi.at[k], {"vol": vol - 1}),
        )
        return [
            (go, remote(src, dst, halo_send.at[k, i], halo_recv.at[k, i], device))
            for i, (go, src, dst, device) in enumerate(pairs)
        ]

    arrives = (row > 0, row < n_row - 1, col > 0, col < n_col - 1, vol > 0, vol < n_vol - 1)

    def halo_start(k):
        copies = halo_copies(k)
        for i in (4, 5, 0, 1, 2, 3):
            @pl.when(copies[i][0])
            def _(copy=copies[i][1]):
                copy.start()

    def halo_wait(k):
        for i, (_, copy) in enumerate(halo_copies(k)):
            @pl.when(arrives[i])
            def _(copy=copy):
                copy.wait_recv()

    def halo_sent(k):
        for go, copy in halo_copies(k):
            @pl.when(go)
            def _(copy=copy):
                copy.wait_send()

    def sweep(k, factor, last, seen=None):
        halo_wait(k)
        for x in range(8):
            b, i = x // 4, x % 4
            low, top = zlo[k, b], zhi[k, b]
            low = pltpu.roll(low, 32 * (3 - i), 1) if i < 3 else low
            top = pltpu.roll(top, (128 - 32 * i) % 128, 1) if i else top
            zmix[0, x] = pltpu.roll(jnp.where(group == 3, low, zrow[k, 1, x]), 32, 1)
            zmix[1, x] = pltpu.roll(jnp.where(group == 0, top, zrow[k, 0, x]), 96, 1)

        @pl.loop(0, 8)
        def _(x):
            packed = (jnp.zeros((8, 128), F32),) * 2
            for y in range(8):
                c = [field[k, x + 1, y + 1, SPANS[b], :] for b in range(4)]
                ups = [pltpu.roll(v, 1, 0) for v in c]
                downs = [pltpu.roll(v, 7, 0) for v in c]
                new = []
                for b in range(4):
                    before = zmix[0, x, y : y + 1, :] if b == 0 else ups[b - 1]
                    after = zmix[1, x, y : y + 1, :] if b == 3 else downs[b + 1]
                    up = jnp.where(sub == 0, before, ups[b])
                    down = jnp.where(sub == 7, after, downs[b])
                    sp = SPANS[b]
                    around = (
                        (field[k, x, y + 1, sp, :] + field[k, x + 2, y + 1, sp, :])
                        + (field[k, x + 1, y, sp, :] + field[k, x + 1, y + 2, sp, :])
                        + (up + down)
                    )
                    new.append(
                        (1.0 - factor) * c[b]
                        + factor * (base[x, y, sp, :] + conduct[x, y, sp, :] * around)
                    )
                if seen is not None:
                    for b in range(4):
                        seen[x, y, SPANS[b], :] = new[b]
                if not last:
                    packed = keep(k + 1, x, y, new, packed)
            if not last:
                zrow[k + 1, 0, x], zrow[k + 1, 1, x] = packed

        if not last:
            pack_rows(k + 1)

    def send_flux(it, ref):
        for s in range(SLOTS):
            place = cells[s]
            picked[s : s + 1, :] = ref[
                place >> 8, (place >> 5) & 7, pl.ds(place & 31, 1), :
            ]
        fluxes = []
        for p in range(2):
            seen = picked[8 * p : 8 * p + 8, :] * mine[p]
            seen = seen + pltpu.roll(seen, 64, 1)
            seen = seen + pltpu.roll(seen, 32, 1)
            fluxes.append(seen - slot[p])
        fsend[it] = jnp.where(group % 2 == 0, fluxes[0], fluxes[1])
        fbuf[it, me] = fsend[it]

        @pl.loop(1, blocks)
        def _(d):
            remote(
                fsend.at[it], fbuf.at[it, me], phase_send.at[2 + it], phase_recv.at[2 + it],
                block_id(block_peer(d)),
            ).start()

    def spread_flux(it):
        whole(fbuf.at[it, pl.ds(0, blocks - 1)], 2 + it).wait_recv()
        seen = fbuf[it].reshape(blocks * 8, 128).astype(BF16)
        dense = jnp.zeros((lead, 128), F32)
        for p in range(2):
            half = select[p * blocks * 8 : (p + 1) * blocks * 8, :]
            every = lax.dot_general(seen, half, TN, preferred_element_type=F32)
            dense += every[lead * p : lead * p + lead, :]
        fall[it, mine_near] = dense.astype(BF16)
        for peer in nears:
            remote(
                fall.at[it, mine_near], fall.at[it, mine_near], phase_send.at[4 + it],
                phase_recv.at[4 + it], {"row": peer},
            ).start()

    def new_share(it, old):
        whole(fall.at[it, pl.ds(0, near - 1)], 4 + it).wait_recv()
        if it == 0:
            whole(strip.at[pl.ds(0, near - 1)], 6).wait_recv()
        for f in range(far):
            update = jnp.zeros((lead, share), F32)
            for n in range(near):
                update += jnp.dot(fall[it, n], strip[n, f], preferred_element_type=F32)
            usend[it, f] = update
        urecv[it, mine_far] = usend[it, mine_far]
        for d in range(1, far):
            f = lax.rem(mine_far + d, far)
            remote(
                usend.at[it, f], urecv.at[it, mine_far], phase_send.at[7 + it],
                phase_recv.at[7 + it], {"row": lax.rem(row + near * d, n_row)},
            ).start()
        if far > 1:
            whole(urecv.at[it, pl.ds(0, far - 1)], 7 + it).wait_recv()
        update = urecv[it, 0]
        for f in range(1, far):
            update += urecv[it, f]
        return old + RELAXATION * update

    right_side(0)
    first_sweep(0, factors[0])
    halo_start(0)
    send_panel(1)
    sweep(0, factors[1], False)
    halo_start(1)
    send_panel(2)
    sweep(1, factors[2], False)
    halo_start(2)
    send_panel(3)
    sweep(2, factors[3], False, middle)
    send_flux(0, middle)
    halo_start(3)
    spread_flux(0)
    state = new_share(0, density[:, own])
    osend[0] = state
    rbuf[row] = state.astype(BF16)

    sent_rounded = gather(0, lambda r: rbuf.at[r])

    send_potential(1, lambda k: rbuf[k])
    right_side(1)
    sweep(3, factors[0], False)
    halo_start(4)
    sweep(4, factors[1], False)
    halo_start(5)
    sweep(5, factors[2], False)
    halo_start(6)
    sweep(6, factors[3], True, inner)
    send_flux(1, inner)

    @pl.loop(0, 16, unroll=TURN)
    def _(i):
        x, y = i // 2, (i % 2) * 4
        tiles = quarters([inner[x, y + q] for q in range(4)])
        back = jnp.transpose(jnp.concatenate(tiles, axis=0))
        for q in range(4):
            volume_out[pl.ds(x * 8 + y + q, lead, stride=64), :] = back[lead * q : lead * q + lead, :]

    spread_flux(1)
    state = new_share(1, osend[0])
    density_out[:, own] = state

    sent_final = gather(
        1, lambda r: density_out.at[:, pl.ds(pl.multiple_of(r * share, share), share)]
    )

    for it in range(OUTER):
        whole(pbuf.at[it, pl.ds(0, blocks - 1)], it).wait_send()
        whole(fbuf.at[it, pl.ds(0, blocks - 1)], 2 + it).wait_send()
        whole(fall.at[it, pl.ds(0, near - 1)], 4 + it).wait_send()
        if far > 1:
            whole(urecv.at[it, pl.ds(0, far - 1)], 7 + it).wait_send()
    whole(strip.at[pl.ds(0, near - 1)], 6).wait_send()
    sent_rounded()
    sent_final()
    for k in range(exchanges):
        halo_sent(k)


def local(panel, density, source, class_index, class_values, trace_count, trace_cell):
    sizes = (lax.axis_size("row"), lax.axis_size("col"), lax.axis_size("vol"))
    n_row, n_col, n_vol = sizes
    blocks = n_col * n_vol
    lead = source.shape[0]
    targets, nodes = panel.shape
    share = nodes // n_row
    near = min(4, n_row)
    ex = SWEEPS * OUTER - 1
    vmem = lambda shape, kind=F32: pltpu.VMEM(shape, kind)
    dma = pltpu.SemaphoreType.DMA
    density_out, volume = pl.pallas_call(
        functools.partial(kernel, sizes),
        out_shape=(
            jax.ShapeDtypeStruct(density.shape, F32),
            jax.ShapeDtypeStruct((lead * 64, 128), F32),
        ),
        in_specs=[pl.BlockSpec(memory_space=pltpu.VMEM)] * 4
        + [pl.BlockSpec(memory_space=pltpu.SMEM)] * 3,
        out_specs=(pl.BlockSpec(memory_space=pltpu.VMEM),) * 2,
        scratch_shapes=[
            vmem((blocks * SLOTS, targets), BF16),
            vmem((2048, 128), BF16),
            vmem((8, 8, 32, 128)),
            vmem((8, 8, 32, 128)),
            vmem((8, 8, 32, 128)),
            vmem((8, 8, 32, 128)),
            vmem((8, 8, 32, 128)),
            vmem((ex, 10, 10, 32, 128)),
            vmem((ex, 2, 2, 8, 128)),
            vmem((ex, 2, 8, 128)),
            vmem((ex, 2, 8, 128)),
            vmem((ex, 2, 8, 8, 128)),
            vmem((2, 8, 8, 128)),
            vmem((64, 128)),
            vmem((2, 8, 128)),
            vmem((SLOTS, 128)),
            vmem((OUTER, blocks, 8, 128)),
            vmem((OUTER, blocks, 8, 128)),
            vmem((OUTER, 8, 128)),
            vmem((OUTER, blocks, 8, 128)),
            vmem((OUTER, near, lead, targets), BF16),
            vmem((near, n_row // near, targets, share), BF16),
            vmem((OUTER, n_row // near, lead, share)),
            vmem((OUTER, n_row // near, lead, share)),
            vmem((n_row, lead, share), BF16),
            vmem((1, lead, share)),
            dma((ex, 6)),
            dma((ex, 6)),
            dma((9,)),
            dma((9,)),
            dma((2, n_row, n_row)),
            dma((2, n_row)),
        ],
        compiler_params=pltpu.CompilerParams(
            collective_id=0, has_side_effects=True, vmem_limit_bytes=56 * 1024 * 1024
        ),
    )(
        panel,
        density,
        source.reshape(lead * 64, 128),
        class_index.reshape(64, 128),
        class_values,
        trace_count,
        trace_cell,
    )
    return density_out, volume.reshape(source.shape)


def solution(mesh):
    placed = (
        P("row", ("col", "vol")),
        P(None, ("col", "vol")),
        P(None, "row", "col", "vol"),
        P("row", "col", "vol"),
        P(),
        P("row", None),
        P("row", None, None),
    )
    return jax.shard_map(
        local,
        mesh=mesh,
        in_specs=placed,
        out_specs=(P(None, ("col", "vol")), P(None, "row", "col", "vol")),
        check_vma=False,
    )
```

```python
import functools
import math

import jax
import jax.numpy as jnp
from jax import lax
from jax.experimental import pallas as pl
from jax.experimental.pallas import tpu as pltpu
from jax.sharding import PartitionSpec as P

SWEEPS = 4
OUTER = 2
MASS_TERM = 0.1
RELAXATION = 0.5
SPECTRUM_LOW = 0.1
SPECTRUM_HIGH = 2.0
MESH = pl.DeviceIdType.MESH
F32 = jnp.float32
BF16 = jnp.bfloat16
NT = (((1,), (1,)), ((), ()))
TN = (((0,), (0,)), ((), ()))
SLOTS = 16
TURN = 4
SPANS = tuple(slice(8 * b, 8 * b + 8) for b in range(4))


def relax_factors(count):
    middle = (SPECTRUM_HIGH + SPECTRUM_LOW) / 2.0
    spread = (SPECTRUM_HIGH - SPECTRUM_LOW) / 2.0
    return [
        1.0 / (middle + spread * math.cos(math.pi * (2 * order + 1) / (2 * count)))
        for order in range(count)
    ]


def kernel(
    sizes,
    panel, density, source, class_index, class_values, trace_count, trace_cell,
    density_out, volume_out,
    select, hits, conduct, inverse, inner, middle, base, field, zface, zlo, zhi, zrow, zmix,
    turned, slot, picked, psend, pbuf, fsend, fbuf, fall, strip, usend, urecv, rbuf, osend,
    halo_send, halo_recv, phase_send, phase_recv, gather_send, gather_recv,
):
    n_row, n_col, n_vol = sizes
    blocks = n_col * n_vol
    share = density.shape[1] // n_row
    lead = density.shape[0]
    factors = relax_factors(SWEEPS)
    row = lax.axis_index("row")
    col = lax.axis_index("col")
    vol = lax.axis_index("vol")
    me = col * n_vol + vol

    def block_id(j):
        return {"col": j // n_vol, "vol": j % n_vol}

    def steps(size):
        return sorted(range(size), key=lambda d: (-min(d, size - d), d))

    block_steps = [(c, v) for v in steps(n_vol) for c in steps(n_col) if (c, v) != (0, 0)]

    def block_peer(step):
        return lax.rem(col + step[0], n_col) * n_vol + lax.rem(vol + step[1], n_vol)

    def row_peer(d):
        return lax.rem(row + d, n_row)

    barrier = pltpu.get_barrier_semaphore()

    for step in block_steps:
        pl.semaphore_signal(
            barrier, inc=1, device_id=block_id(block_peer(step)), device_id_type=MESH
        )

    @pl.loop(1, n_row)
    def _(d):
        pl.semaphore_signal(barrier, inc=1, device_id={"row": row_peer(d)}, device_id_type=MESH)

    def remote(src, dst, send, recv, device):
        return pltpu.make_async_remote_copy(
            src_ref=src, dst_ref=dst, send_sem=send, recv_sem=recv,
            device_id=device, device_id_type=MESH,
        )

    def whole(ref, phase):
        return remote(ref, ref, phase_send.at[phase], phase_recv.at[phase], {"row": row})

    sub = lax.broadcasted_iota(jnp.int32, (8, 128), 0)
    lane = lax.broadcasted_iota(jnp.int32, (8, 128), 1)
    group = lane // 32
    exchanges = field.shape[0]

    def pieces(x):
        first = x.astype(BF16)
        rest = x - first.astype(F32)
        second = rest.astype(BF16)
        third = (rest - second.astype(F32)).astype(BF16)
        return first, second, third

    offset = jnp.int32(0)
    marks = []
    for j in range(blocks):
        count = trace_count[0, j]
        marks.append((offset, count))
        offset = offset + count
    for p in range(2):
        for j in range(0, blocks, 2):
            both = []
            for start, count in marks[j : j + 2]:
                s = sub + 8 * p
                both.append(jnp.where((lane == s + start) & (s < count), 1.0, 0.0).astype(F32))
            at = p * blocks * 8 + j * 8
            select[at : at + 16, :] = jnp.concatenate(both, axis=0).astype(BF16)

    def quarters(tiles):
        a = list(tiles)
        grp = lax.broadcasted_iota(jnp.int32, a[0].shape, 1) // 32
        for step in (2, 1):
            out = list(a)
            for i in range(4):
                if i & step == 0:
                    j = i | step
                    shift = 32 * step
                    keep = (grp & step) == 0
                    out[i] = jnp.where(keep, a[i], pltpu.roll(a[j], shift, 1))
                    out[j] = jnp.where(keep, pltpu.roll(a[i], 128 - shift, 1), a[j])
            a = out
        return a

    def to_inner(rows, write):
        @pl.loop(0, 16, unroll=TURN)
        def _(i):
            x, y = i // 2, (i % 2) * 4
            stacked = jnp.concatenate([rows(x, y + q) for q in range(4)], axis=0)
            flipped = jnp.transpose(stacked)
            for q, tile in enumerate(quarters([flipped[32 * q : 32 * q + 32, :] for q in range(4)])):
                write(x, y + q, tile)

    cls = class_index[...]
    value = jnp.zeros(cls.shape, F32)
    for k in range(class_values.shape[0]):
        value = jnp.where(cls == k, class_values[k], value)
    turned[...] = value

    def coefficients(x, y, tile):
        inv = 1.0 / (MASS_TERM + 6.0 * tile)
        inverse[x, y] = inv
        conduct[x, y] = tile * inv

    def prepare():
        to_inner(
            lambda x, y: jnp.broadcast_to(turned[pl.ds(x * 8 + y, 1), :], (lead, 128)), coefficients
        )

    def send_potential(it, chunk):
        partial = jnp.zeros((panel.shape[0], 128), F32)
        for k in range(n_row):
            part = chunk(k)
            partial += lax.dot_general(
                panel[:, k * share : (k + 1) * share],
                jnp.concatenate([part] * (128 // lead), axis=0),
                NT, preferred_element_type=F32,
            )
        chosen = jnp.zeros((select.shape[0], 128), F32)
        for piece in pieces(partial):
            chosen += jnp.dot(select[...], piece, preferred_element_type=F32)
        half = blocks * 8
        for j in range(blocks):
            psend[it, j] = jnp.where(
                group % 2 == 0, chosen[8 * j : 8 * j + 8, :],
                chosen[half + 8 * j : half + 8 * j + 8, :],
            )
        if it == 0:
            prepare()
            pl.semaphore_wait(barrier, blocks - 1 + n_row - 1)
        pbuf[it, me] = psend[it, me]

        for step in block_steps:
            j = block_peer(step)
            remote(
                psend.at[it, j], pbuf.at[it, me], phase_send.at[it], phase_recv.at[it], block_id(j)
            ).start()

    near = min(4, n_row)
    far = n_row // near

    base_row = row - lax.rem(row, near)
    mine_near = lax.rem(row, near)
    mine_far = row // near
    nears = [base_row + lax.rem(row + d, near) for d in range(1, near)]
    fars = [lax.rem(row + near * d, n_row) for d in range(1, far)]

    def panel_copy(d, f):
        r = base_row + lax.rem(row + d, near)
        at = (near * f + lax.rem(r, near)) * share
        return remote(
            panel.at[:, pl.ds(pl.multiple_of(at, share), share)], strip.at[mine_near, f],
            phase_send.at[6], phase_recv.at[6], {"row": r},
        )

    chunks = [(d, f) for f in range(far) for d in range(1, near)]
    cuts = [len(chunks) * part // 12 for part in (0, 6, 8, 10, 12)]

    def send_panel(i):
        for d, f in chunks[cuts[i] : cuts[i + 1]]:
            panel_copy(d, f).start()

    def gather(i, cut):
        def copy(r, peer):
            return remote(
                cut(r), cut(r), gather_send.at[i, r, peer], gather_recv.at[i, r], {"row": peer}
            )

        for peer in fars + nears:
            copy(row, peer).start()
        for r in fars:
            copy(r, row).wait_recv()
            for peer in nears:
                copy(r, peer).start()
        for peer in nears:
            for q in range(far):
                copy(lax.rem(peer + near * q, n_row), row).wait_recv()

        def sent():
            for peer in fars + nears:
                copy(row, peer).wait_send()
            for r in fars:
                for peer in nears:
                    copy(r, peer).wait_send()

        return sent

    own = pl.ds(pl.multiple_of(row * share, share), share)
    send_potential(0, lambda k: density[:, k * share : (k + 1) * share].astype(BF16))
    for f in range(far):
        at = (near * f + mine_near) * share
        strip[mine_near, f] = panel[:, pl.ds(pl.multiple_of(at, share), share)]
    send_panel(0)

    own_count = trace_count[0, me]
    cells, spot = [], jnp.full((8, 128), -1, jnp.int32)
    quarter = [jnp.full((8, 128), -1, jnp.int32) for _ in range(2)]
    for s in range(SLOTS):
        cell = jnp.where(s < own_count, trace_cell[0, me, s], -1)
        place = (cell >> 7) * 32 + (cell & 31)
        spot = jnp.where(lane % SLOTS == s, jnp.where(cell >= 0, place, -1), spot)
        fourth = jnp.where(cell >= 0, (cell >> 5) & 3, -1)
        quarter[s // 8] = jnp.where(sub == s % 8, fourth, quarter[s // 8])
        cells.append(jnp.maximum(place, 0))
    mine = [jnp.where(quarter[p] == group, 1.0, 0.0).astype(F32) for p in range(2)]
    spot = jnp.where(lane < 3 * SLOTS, spot, -1)

    @pl.loop(0, 128)
    def _(i):
        at = pl.multiple_of(i * 16, 16)
        here = jnp.concatenate([sub, sub + 8], axis=0) + at
        wide = jnp.concatenate([spot, spot], axis=0)
        hits[pl.ds(at, 16), :] = jnp.where(here == wide, 1.0, 0.0).astype(BF16)

    def keep_source(x, y, tile):
        inner[x, y] = tile

    to_inner(lambda x, y: source[pl.ds(x * 8 + y, lead, stride=64), :], keep_source)

    def clear(write):
        @pl.loop(0, exchanges)
        def _(k):
            write(k)

    def clear_x(k, x):
        field[k, x] = jnp.zeros(field.shape[2:], F32)

    def clear_y(k, y):
        @pl.loop(0, 10)
        def _(x):
            field[k, x, y] = jnp.zeros(field.shape[3:], F32)

    def clear_z(ref, k):
        ref[k] = jnp.zeros(ref.shape[1:], F32)

    for here, edge, write in (
        (row, 0, lambda k: clear_x(k, 0)), (row, n_row - 1, lambda k: clear_x(k, 9)),
        (col, 0, lambda k: clear_y(k, 0)), (col, n_col - 1, lambda k: clear_y(k, 9)),
        (vol, 0, lambda k: clear_z(zlo, k)), (vol, n_vol - 1, lambda k: clear_z(zhi, k)),
    ):
        @pl.when(here == edge)
        def _(write=write):
            clear(write)

    def right_side(it):
        whole(pbuf.at[it, pl.ds(0, blocks - 1)], it).wait_recv()
        total = pbuf[it, 0]
        for j in range(1, blocks):
            total += pbuf[it, j]
        swapped = pltpu.roll(total, 32, 1)
        even = group % 2 == 0
        parts = [jnp.where(even, total, swapped), jnp.where(even, swapped, total)]
        for p in range(2):
            slot[p] = parts[p]
        placed = jnp.concatenate([parts[p] * mine[p] for p in range(2)], axis=0)
        values = jnp.concatenate(
            list(pieces(placed)) + [jnp.zeros((128 - 3 * SLOTS, 128), BF16)], axis=0
        )

        @pl.loop(0, 8)
        def _(x):
            at = pl.multiple_of(x * 256, 256)
            added = jnp.dot(hits[pl.ds(at, 256), :], values, preferred_element_type=F32)
            for y in range(8):
                base[x, y] = (inner[x, y] + added[32 * y : 32 * y + 32, :]) * inverse[x, y]

    def keep(k, x, y, new, packed):
        low, top = packed
        for b in range(4):
            field[k, x + 1, y + 1, SPANS[b], :] = new[b]
        low = jnp.where(sub == y, pltpu.roll(new[0], y, 0) if y else new[0], low)
        top = jnp.where(sub == y, pltpu.roll(new[3], y + 1, 0) if y < 7 else new[3], top)
        return low, top

    def pack_rows(k):
        for side, edge in ((0, 0), (1, 3)):
            for b in range(2):
                packed = jnp.zeros((8, 128), F32)
                for i in range(4):
                    moved = zrow[k, side, 4 * b + i]
                    if i != edge:
                        moved = pltpu.roll(moved, (32 * (i - edge)) % 128, 1)
                    packed = jnp.where(group == i, moved, packed)
                zface[k, side, b] = packed

    def ends_first(plane, between):
        @pl.loop(0, 2)
        def _(i):
            plane(7 * i)

        between()

        @pl.loop(1, 7)
        def _(x):
            plane(x)

    def first_sweep(k, factor):
        def plane(x):
            packed = (jnp.zeros((8, 128), F32),) * 2
            for y in range(8):
                new = [factor * base[x, y, SPANS[b], :] for b in range(4)]
                packed = keep(k, x, y, new, packed)
            zrow[k, 0, x], zrow[k, 1, x] = packed

        ends_first(plane, lambda: halo_start(k, (0, 1)))
        pack_rows(k)
        halo_start(k, (4, 5, 2, 3))

    def halo_copies(k):
        pairs = (
            (row < n_row - 1, field.at[k, 8, pl.ds(1, 8)], field.at[k, 0, pl.ds(1, 8)], {"row": row + 1}),
            (row > 0, field.at[k, 1, pl.ds(1, 8)], field.at[k, 9, pl.ds(1, 8)], {"row": row - 1}),
            (col < n_col - 1, field.at[k, pl.ds(1, 8), 8], field.at[k, pl.ds(1, 8), 0], {"col": col + 1}),
            (col > 0, field.at[k, pl.ds(1, 8), 1], field.at[k, pl.ds(1, 8), 9], {"col": col - 1}),
            (vol < n_vol - 1, zface.at[k, 1], zlo.at[k], {"vol": vol + 1}),
            (vol > 0, zface.at[k, 0], zhi.at[k], {"vol": vol - 1}),
        )
        return [
            (go, remote(src, dst, halo_send.at[k, i], halo_recv.at[k, i], device))
            for i, (go, src, dst, device) in enumerate(pairs)
        ]

    arrives = (row > 0, row < n_row - 1, col > 0, col < n_col - 1, vol > 0, vol < n_vol - 1)

    def halo_start(k, which):
        copies = halo_copies(k)
        for i in which:
            @pl.when(copies[i][0])
            def _(copy=copies[i][1]):
                copy.start()

    def halo_wait(k):
        for i, (_, copy) in enumerate(halo_copies(k)):
            @pl.when(arrives[i])
            def _(copy=copy):
                copy.wait_recv()

    def halo_sent(k):
        for go, copy in halo_copies(k):
            @pl.when(go)
            def _(copy=copy):
                copy.wait_send()

    def sweep(k, factor, last, seen=None):
        halo_wait(k)
        for x in range(8):
            b, i = x // 4, x % 4
            low, top = zlo[k, b], zhi[k, b]
            low = pltpu.roll(low, 32 * (3 - i), 1) if i < 3 else low
            top = pltpu.roll(top, (128 - 32 * i) % 128, 1) if i else top
            zmix[0, x] = pltpu.roll(jnp.where(group == 3, low, zrow[k, 1, x]), 32, 1)
            zmix[1, x] = pltpu.roll(jnp.where(group == 0, top, zrow[k, 0, x]), 96, 1)

        def plane(x):
            packed = (jnp.zeros((8, 128), F32),) * 2
            for y in range(8):
                c = [field[k, x + 1, y + 1, SPANS[b], :] for b in range(4)]
                ups = [pltpu.roll(v, 1, 0) for v in c]
                downs = [pltpu.roll(v, 7, 0) for v in c]
                new = []
                for b in range(4):
                    before = zmix[0, x, y : y + 1, :] if b == 0 else ups[b - 1]
                    after = zmix[1, x, y : y + 1, :] if b == 3 else downs[b + 1]
                    up = jnp.where(sub == 0, before, ups[b])
                    down = jnp.where(sub == 7, after, downs[b])
                    sp = SPANS[b]
                    around = (
                        (field[k, x, y + 1, sp, :] + field[k, x + 2, y + 1, sp, :])
                        + (field[k, x + 1, y, sp, :] + field[k, x + 1, y + 2, sp, :])
                        + (up + down)
                    )
                    new.append(
                        (1.0 - factor) * c[b]
                        + factor * (base[x, y, sp, :] + conduct[x, y, sp, :] * around)
                    )
                if seen is not None:
                    for b in range(4):
                        seen[x, y, SPANS[b], :] = new[b]
                if not last:
                    packed = keep(k + 1, x, y, new, packed)
            if not last:
                zrow[k + 1, 0, x], zrow[k + 1, 1, x] = packed

        if last:
            pl.loop(0, 8)(plane)
        else:
            ends_first(plane, lambda: halo_start(k + 1, (0, 1)))
            pack_rows(k + 1)
            if seen is None:
                halo_start(k + 1, (4, 5, 2, 3))

    def send_flux(it, ref):
        for s in range(SLOTS):
            place = cells[s]
            picked[s : s + 1, :] = ref[
                place >> 8, (place >> 5) & 7, pl.ds(place & 31, 1), :
            ]
        fluxes = []
        for p in range(2):
            seen = picked[8 * p : 8 * p + 8, :] * mine[p]
            seen = seen + pltpu.roll(seen, 64, 1)
            seen = seen + pltpu.roll(seen, 32, 1)
            fluxes.append(seen - slot[p])
        fsend[it] = jnp.where(group % 2 == 0, fluxes[0], fluxes[1])
        fbuf[it, me] = fsend[it]

        for step in block_steps:
            remote(
                fsend.at[it], fbuf.at[it, me], phase_send.at[2 + it], phase_recv.at[2 + it],
                block_id(block_peer(step)),
            ).start()

    def spread_flux(it):
        whole(fbuf.at[it, pl.ds(0, blocks - 1)], 2 + it).wait_recv()
        seen = fbuf[it].reshape(blocks * 8, 128).astype(BF16)
        dense = jnp.zeros((lead, 128), F32)
        for p in range(2):
            half = select[p * blocks * 8 : (p + 1) * blocks * 8, :]
            every = lax.dot_general(seen, half, TN, preferred_element_type=F32)
            dense += every[lead * p : lead * p + lead, :]
        fall[it, mine_near] = dense.astype(BF16)
        for peer in nears:
            remote(
                fall.at[it, mine_near], fall.at[it, mine_near], phase_send.at[4 + it],
                phase_recv.at[4 + it], {"row": peer},
            ).start()

    def new_share(it, old):
        whole(fall.at[it, pl.ds(0, near - 1)], 4 + it).wait_recv()
        if it == 0:
            whole(strip.at[pl.ds(0, near - 1)], 6).wait_recv()
        for f in range(far):
            update = jnp.zeros((lead, share), F32)
            for n in range(near):
                update += jnp.dot(fall[it, n], strip[n, f], preferred_element_type=F32)
            usend[it, f] = update
        urecv[it, mine_far] = usend[it, mine_far]
        for d in range(1, far):
            f = lax.rem(mine_far + d, far)
            remote(
                usend.at[it, f], urecv.at[it, mine_far], phase_send.at[7 + it],
                phase_recv.at[7 + it], {"row": lax.rem(row + near * d, n_row)},
            ).start()
        if far > 1:
            whole(urecv.at[it, pl.ds(0, far - 1)], 7 + it).wait_recv()
        update = urecv[it, 0]
        for f in range(1, far):
            update += urecv[it, f]
        return old + RELAXATION * update

    right_side(0)
    first_sweep(0, factors[0])
    send_panel(1)
    sweep(0, factors[1], False)
    send_panel(2)
    sweep(1, factors[2], False)
    send_panel(3)
    sweep(2, factors[3], False, middle)
    send_flux(0, middle)
    halo_start(3, (4, 5, 2, 3))
    spread_flux(0)
    state = new_share(0, density[:, own])
    osend[0] = state
    rbuf[row] = state.astype(BF16)

    sent_rounded = gather(0, lambda r: rbuf.at[r])

    send_potential(1, lambda k: rbuf[k])
    right_side(1)
    sweep(3, factors[0], False)
    sweep(4, factors[1], False)
    sweep(5, factors[2], False)
    sweep(6, factors[3], True, inner)
    send_flux(1, inner)

    @pl.loop(0, 16, unroll=TURN)
    def _(i):
        x, y = i // 2, (i % 2) * 4
        tiles = quarters([inner[x, y + q] for q in range(4)])
        back = jnp.transpose(jnp.concatenate(tiles, axis=0))
        for q in range(4):
            volume_out[pl.ds(x * 8 + y + q, lead, stride=64), :] = back[lead * q : lead * q + lead, :]

    spread_flux(1)
    state = new_share(1, osend[0])
    density_out[:, own] = state

    sent_final = gather(
        1, lambda r: density_out.at[:, pl.ds(pl.multiple_of(r * share, share), share)]
    )

    for it in range(OUTER):
        whole(pbuf.at[it, pl.ds(0, blocks - 1)], it).wait_send()
        whole(fbuf.at[it, pl.ds(0, blocks - 1)], 2 + it).wait_send()
        whole(fall.at[it, pl.ds(0, near - 1)], 4 + it).wait_send()
        if far > 1:
            whole(urecv.at[it, pl.ds(0, far - 1)], 7 + it).wait_send()
    whole(strip.at[pl.ds(0, near - 1)], 6).wait_send()
    sent_rounded()
    sent_final()
    for k in range(exchanges):
        halo_sent(k)


def local(panel, density, source, class_index, class_values, trace_count, trace_cell):
    sizes = (lax.axis_size("row"), lax.axis_size("col"), lax.axis_size("vol"))
    n_row, n_col, n_vol = sizes
    blocks = n_col * n_vol
    lead = source.shape[0]
    targets, nodes = panel.shape
    share = nodes // n_row
    near = min(4, n_row)
    ex = SWEEPS * OUTER - 1
    vmem = lambda shape, kind=F32: pltpu.VMEM(shape, kind)
    dma = pltpu.SemaphoreType.DMA
    density_out, volume = pl.pallas_call(
        functools.partial(kernel, sizes),
        out_shape=(
            jax.ShapeDtypeStruct(density.shape, F32),
            jax.ShapeDtypeStruct((lead * 64, 128), F32),
        ),
        in_specs=[pl.BlockSpec(memory_space=pltpu.VMEM)] * 4
        + [pl.BlockSpec(memory_space=pltpu.SMEM)] * 3,
        out_specs=(pl.BlockSpec(memory_space=pltpu.VMEM),) * 2,
        scratch_shapes=[
            vmem((blocks * SLOTS, targets), BF16),
            vmem((2048, 128), BF16),
            vmem((8, 8, 32, 128)),
            vmem((8, 8, 32, 128)),
            vmem((8, 8, 32, 128)),
            vmem((8, 8, 32, 128)),
            vmem((8, 8, 32, 128)),
            vmem((ex, 10, 10, 32, 128)),
            vmem((ex, 2, 2, 8, 128)),
            vmem((ex, 2, 8, 128)),
            vmem((ex, 2, 8, 128)),
            vmem((ex, 2, 8, 8, 128)),
            vmem((2, 8, 8, 128)),
            vmem((64, 128)),
            vmem((2, 8, 128)),
            vmem((SLOTS, 128)),
            vmem((OUTER, blocks, 8, 128)),
            vmem((OUTER, blocks, 8, 128)),
            vmem((OUTER, 8, 128)),
            vmem((OUTER, blocks, 8, 128)),
            vmem((OUTER, near, lead, targets), BF16),
            vmem((near, n_row // near, targets, share), BF16),
            vmem((OUTER, n_row // near, lead, share)),
            vmem((OUTER, n_row // near, lead, share)),
            vmem((n_row, lead, share), BF16),
            vmem((1, lead, share)),
            dma((ex, 6)),
            dma((ex, 6)),
            dma((9,)),
            dma((9,)),
            dma((2, n_row, n_row)),
            dma((2, n_row)),
        ],
        compiler_params=pltpu.CompilerParams(
            collective_id=0, has_side_effects=True, vmem_limit_bytes=56 * 1024 * 1024
        ),
    )(
        panel,
        density,
        source.reshape(lead * 64, 128),
        class_index.reshape(64, 128),
        class_values,
        trace_count,
        trace_cell,
    )
    return density_out, volume.reshape(source.shape)


def solution(mesh):
    placed = (
        P("row", ("col", "vol")),
        P(None, ("col", "vol")),
        P(None, "row", "col", "vol"),
        P("row", "col", "vol"),
        P(),
        P("row", None),
        P("row", None, None),
    )
    return jax.shard_map(
        local,
        mesh=mesh,
        in_specs=placed,
        out_specs=(P(None, ("col", "vol")), P(None, "row", "col", "vol")),
        check_vma=False,
    )
```

```python
import functools
import math

import jax
import jax.numpy as jnp
from jax import lax
from jax.experimental import pallas as pl
from jax.experimental.pallas import tpu as pltpu
from jax.sharding import PartitionSpec as P

SWEEPS = 4
OUTER = 2
MASS_TERM = 0.1
RELAXATION = 0.5
SPECTRUM_LOW = 0.1
SPECTRUM_HIGH = 2.0
MESH = pl.DeviceIdType.MESH
F32 = jnp.float32
BF16 = jnp.bfloat16
NT = (((1,), (1,)), ((), ()))
TN = (((0,), (0,)), ((), ()))
SLOTS = 16
TURN = 4
SPANS = tuple(slice(8 * b, 8 * b + 8) for b in range(4))


def relax_factors(count):
    middle = (SPECTRUM_HIGH + SPECTRUM_LOW) / 2.0
    spread = (SPECTRUM_HIGH - SPECTRUM_LOW) / 2.0
    return [
        1.0 / (middle + spread * math.cos(math.pi * (2 * order + 1) / (2 * count)))
        for order in range(count)
    ]


def kernel(
    sizes,
    panel, density, source, class_index, class_values, trace_count, trace_cell,
    density_out, volume_out,
    select, hits, conduct, inverse, inner, middle, base, field, zface, zlo, zhi, zrow, zmix,
    turned, slot, picked, psend, pbuf, fsend, fbuf, fall, strip, usend, urecv, rbuf, osend,
    halo_send, halo_recv, phase_send, phase_recv, gather_send, gather_recv,
):
    n_row, n_col, n_vol = sizes
    blocks = n_col * n_vol
    share = density.shape[1] // n_row
    lead = density.shape[0]
    factors = relax_factors(SWEEPS)
    row = lax.axis_index("row")
    col = lax.axis_index("col")
    vol = lax.axis_index("vol")
    me = col * n_vol + vol

    def block_id(j):
        return {"col": j // n_vol, "vol": j % n_vol}

    def block_peer(d):
        return lax.rem(me + d, blocks)

    def row_peer(d):
        return lax.rem(row + d, n_row)

    barrier = pltpu.get_barrier_semaphore()

    @pl.loop(1, blocks)
    def _(d):
        pl.semaphore_signal(barrier, inc=1, device_id=block_id(block_peer(d)), device_id_type=MESH)

    @pl.loop(1, n_row)
    def _(d):
        pl.semaphore_signal(barrier, inc=1, device_id={"row": row_peer(d)}, device_id_type=MESH)

    def remote(src, dst, send, recv, device):
        return pltpu.make_async_remote_copy(
            src_ref=src, dst_ref=dst, send_sem=send, recv_sem=recv,
            device_id=device, device_id_type=MESH,
        )

    def whole(ref, phase):
        return remote(ref, ref, phase_send.at[phase], phase_recv.at[phase], {"row": row})

    sub = lax.broadcasted_iota(jnp.int32, (8, 128), 0)
    lane = lax.broadcasted_iota(jnp.int32, (8, 128), 1)
    group = lane // 32
    exchanges = field.shape[0]

    def pieces(x):
        first = x.astype(BF16)
        rest = x - first.astype(F32)
        second = rest.astype(BF16)
        third = (rest - second.astype(F32)).astype(BF16)
        return first, second, third

    offset = jnp.int32(0)
    marks = []
    for j in range(blocks):
        count = trace_count[0, j]
        marks.append((offset, count))
        offset = offset + count
    for p in range(2):
        for j in range(0, blocks, 2):
            both = []
            for start, count in marks[j : j + 2]:
                s = sub + 8 * p
                both.append(jnp.where((lane == s + start) & (s < count), 1.0, 0.0).astype(F32))
            at = p * blocks * 8 + j * 8
            select[at : at + 16, :] = jnp.concatenate(both, axis=0).astype(BF16)

    def quarters(tiles):
        a = list(tiles)
        grp = lax.broadcasted_iota(jnp.int32, a[0].shape, 1) // 32
        for step in (2, 1):
            out = list(a)
            for i in range(4):
                if i & step == 0:
                    j = i | step
                    shift = 32 * step
                    keep = (grp & step) == 0
                    out[i] = jnp.where(keep, a[i], pltpu.roll(a[j], shift, 1))
                    out[j] = jnp.where(keep, pltpu.roll(a[i], 128 - shift, 1), a[j])
            a = out
        return a

    def to_inner(rows, write):
        @pl.loop(0, 16, unroll=TURN)
        def _(i):
            x, y = i // 2, (i % 2) * 4
            stacked = jnp.concatenate([rows(x, y + q) for q in range(4)], axis=0)
            flipped = jnp.transpose(stacked)
            for q, tile in enumerate(quarters([flipped[32 * q : 32 * q + 32, :] for q in range(4)])):
                write(x, y + q, tile)

    cls = class_index[...]
    value = jnp.zeros(cls.shape, F32)
    for k in range(class_values.shape[0]):
        value = jnp.where(cls == k, class_values[k], value)
    turned[...] = value

    def coefficients(x, y, tile):
        inv = 1.0 / (MASS_TERM + 6.0 * tile)
        inverse[x, y] = inv
        conduct[x, y] = tile * inv

    def prepare():
        to_inner(
            lambda x, y: jnp.broadcast_to(turned[pl.ds(x * 8 + y, 1), :], (lead, 128)), coefficients
        )

    def send_potential(it, chunk):
        partial = jnp.zeros((panel.shape[0], 128), F32)
        for k in range(n_row):
            part = chunk(k)
            partial += lax.dot_general(
                panel[:, k * share : (k + 1) * share],
                jnp.concatenate([part] * (128 // lead), axis=0),
                NT, preferred_element_type=F32,
            )
        chosen = jnp.zeros((select.shape[0], 128), F32)
        for piece in pieces(partial):
            chosen += jnp.dot(select[...], piece, preferred_element_type=F32)
        half = blocks * 8
        for j in range(blocks):
            psend[it, j] = jnp.where(
                group % 2 == 0, chosen[8 * j : 8 * j + 8, :],
                chosen[half + 8 * j : half + 8 * j + 8, :],
            )
        if it == 0:
            prepare()
            pl.semaphore_wait(barrier, blocks - 1 + n_row - 1)
        pbuf[it, me] = psend[it, me]

        @pl.loop(1, blocks)
        def _(d):
            j = block_peer(d)
            remote(
                psend.at[it, j], pbuf.at[it, me], phase_send.at[it], phase_recv.at[it], block_id(j)
            ).start()

    near = min(4, n_row)
    far = n_row // near

    base_row = row - lax.rem(row, near)
    mine_near = lax.rem(row, near)
    mine_far = row // near
    nears = [base_row + lax.rem(row + d, near) for d in range(1, near)]
    fars = [lax.rem(row + near * d, n_row) for d in range(1, far)]

    def panel_copy(d, f):
        r = base_row + lax.rem(row + d, near)
        at = (near * f + lax.rem(r, near)) * share
        return remote(
            panel.at[:, pl.ds(pl.multiple_of(at, share), share)], strip.at[mine_near, f],
            phase_send.at[6], phase_recv.at[6], {"row": r},
        )

    chunks = [(d, f) for f in range(far) for d in range(1, near)]
    per = (len(chunks) + 3) // 4

    def send_panel(i):
        for d, f in chunks[i * per : (i + 1) * per]:
            panel_copy(d, f).start()

    def gather(i, cut):
        def copy(r, peer):
            return remote(
                cut(r), cut(r), gather_send.at[i, r, peer], gather_recv.at[i, r], {"row": peer}
            )

        for peer in fars + nears:
            copy(row, peer).start()
        for r in fars:
            copy(r, row).wait_recv()
            for peer in nears:
                copy(r, peer).start()
        for peer in nears:
            for q in range(far):
                copy(lax.rem(peer + near * q, n_row), row).wait_recv()

        def sent():
            for peer in fars + nears:
                copy(row, peer).wait_send()
            for r in fars:
                for peer in nears:
                    copy(r, peer).wait_send()

        return sent

    own = pl.ds(pl.multiple_of(row * share, share), share)
    send_potential(0, lambda k: density[:, k * share : (k + 1) * share].astype(BF16))
    for f in range(far):
        at = (near * f + mine_near) * share
        strip[mine_near, f] = panel[:, pl.ds(pl.multiple_of(at, share), share)]
    send_panel(0)

    own_count = trace_count[0, me]
    cells, spot = [], jnp.full((8, 128), -1, jnp.int32)
    quarter = [jnp.full((8, 128), -1, jnp.int32) for _ in range(2)]
    for s in range(SLOTS):
        cell = jnp.where(s < own_count, trace_cell[0, me, s], -1)
        place = (cell >> 7) * 32 + (cell & 31)
        spot = jnp.where(lane % SLOTS == s, jnp.where(cell >= 0, place, -1), spot)
        fourth = jnp.where(cell >= 0, (cell >> 5) & 3, -1)
        quarter[s // 8] = jnp.where(sub == s % 8, fourth, quarter[s // 8])
        cells.append(jnp.maximum(place, 0))
    mine = [jnp.where(quarter[p] == group, 1.0, 0.0).astype(F32) for p in range(2)]
    spot = jnp.where(lane < 3 * SLOTS, spot, -1)

    @pl.loop(0, 128)
    def _(i):
        at = pl.multiple_of(i * 16, 16)
        here = jnp.concatenate([sub, sub + 8], axis=0) + at
        wide = jnp.concatenate([spot, spot], axis=0)
        hits[pl.ds(at, 16), :] = jnp.where(here == wide, 1.0, 0.0).astype(BF16)

    def keep_source(x, y, tile):
        inner[x, y] = tile

    to_inner(lambda x, y: source[pl.ds(x * 8 + y, lead, stride=64), :], keep_source)

    def clear(write):
        @pl.loop(0, exchanges)
        def _(k):
            write(k)

    def clear_x(k, x):
        field[k, x] = jnp.zeros(field.shape[2:], F32)

    def clear_y(k, y):
        @pl.loop(0, 10)
        def _(x):
            field[k, x, y] = jnp.zeros(field.shape[3:], F32)

    def clear_z(ref, k):
        ref[k] = jnp.zeros(ref.shape[1:], F32)

    for here, edge, write in (
        (row, 0, lambda k: clear_x(k, 0)), (row, n_row - 1, lambda k: clear_x(k, 9)),
        (col, 0, lambda k: clear_y(k, 0)), (col, n_col - 1, lambda k: clear_y(k, 9)),
        (vol, 0, lambda k: clear_z(zlo, k)), (vol, n_vol - 1, lambda k: clear_z(zhi, k)),
    ):
        @pl.when(here == edge)
        def _(write=write):
            clear(write)

    def right_side(it):
        whole(pbuf.at[it, pl.ds(0, blocks - 1)], it).wait_recv()
        total = pbuf[it, 0]
        for j in range(1, blocks):
            total += pbuf[it, j]
        swapped = pltpu.roll(total, 32, 1)
        even = group % 2 == 0
        parts = [jnp.where(even, total, swapped), jnp.where(even, swapped, total)]
        for p in range(2):
            slot[p] = parts[p]
        placed = jnp.concatenate([parts[p] * mine[p] for p in range(2)], axis=0)
        values = jnp.concatenate(
            list(pieces(placed)) + [jnp.zeros((128 - 3 * SLOTS, 128), BF16)], axis=0
        )

        @pl.loop(0, 8)
        def _(x):
            at = pl.multiple_of(x * 256, 256)
            added = jnp.dot(hits[pl.ds(at, 256), :], values, preferred_element_type=F32)
            for y in range(8):
                base[x, y] = (inner[x, y] + added[32 * y : 32 * y + 32, :]) * inverse[x, y]

    def keep(k, x, y, new, packed):
        low, top = packed
        for b in range(4):
            field[k, x + 1, y + 1, SPANS[b], :] = new[b]
        low = jnp.where(sub == y, pltpu.roll(new[0], y, 0) if y else new[0], low)
        top = jnp.where(sub == y, pltpu.roll(new[3], y + 1, 0) if y < 7 else new[3], top)
        return low, top

    def pack_rows(k):
        for side, edge in ((0, 0), (1, 3)):
            for b in range(2):
                packed = jnp.zeros((8, 128), F32)
                for i in range(4):
                    moved = zrow[k, side, 4 * b + i]
                    if i != edge:
                        moved = pltpu.roll(moved, (32 * (i - edge)) % 128, 1)
                    packed = jnp.where(group == i, moved, packed)
                zface[k, side, b] = packed

    def ends_first(plane, between):
        @pl.loop(0, 2)
        def _(i):
            plane(7 * i)

        between()

        @pl.loop(1, 7)
        def _(x):
            plane(x)

    def first_sweep(k, factor):
        def plane(x):
            packed = (jnp.zeros((8, 128), F32),) * 2
            for y in range(8):
                new = [factor * base[x, y, SPANS[b], :] for b in range(4)]
                packed = keep(k, x, y, new, packed)
            zrow[k, 0, x], zrow[k, 1, x] = packed

        ends_first(plane, lambda: halo_start(k, (0, 1)))
        pack_rows(k)
        halo_start(k, (4, 5, 2, 3))

    def halo_copies(k):
        pairs = (
            (row < n_row - 1, field.at[k, 8, pl.ds(1, 8)], field.at[k, 0, pl.ds(1, 8)], {"row": row + 1}),
            (row > 0, field.at[k, 1, pl.ds(1, 8)], field.at[k, 9, pl.ds(1, 8)], {"row": row - 1}),
            (col < n_col - 1, field.at[k, pl.ds(1, 8), 8], field.at[k, pl.ds(1, 8), 0], {"col": col + 1}),
            (col > 0, field.at[k, pl.ds(1, 8), 1], field.at[k, pl.ds(1, 8), 9], {"col": col - 1}),
            (vol < n_vol - 1, zface.at[k, 1], zlo.at[k], {"vol": vol + 1}),
            (vol > 0, zface.at[k, 0], zhi.at[k], {"vol": vol - 1}),
        )
        return [
            (go, remote(src, dst, halo_send.at[k, i], halo_recv.at[k, i], device))
            for i, (go, src, dst, device) in enumerate(pairs)
        ]

    arrives = (row > 0, row < n_row - 1, col > 0, col < n_col - 1, vol > 0, vol < n_vol - 1)

    def halo_start(k, which):
        copies = halo_copies(k)
        for i in which:
            @pl.when(copies[i][0])
            def _(copy=copies[i][1]):
                copy.start()

    def halo_wait(k):
        for i, (_, copy) in enumerate(halo_copies(k)):
            @pl.when(arrives[i])
            def _(copy=copy):
                copy.wait_recv()

    def halo_sent(k):
        for go, copy in halo_copies(k):
            @pl.when(go)
            def _(copy=copy):
                copy.wait_send()

    def sweep(k, factor, last, seen=None):
        halo_wait(k)
        for x in range(8):
            b, i = x // 4, x % 4
            low, top = zlo[k, b], zhi[k, b]
            low = pltpu.roll(low, 32 * (3 - i), 1) if i < 3 else low
            top = pltpu.roll(top, (128 - 32 * i) % 128, 1) if i else top
            zmix[0, x] = pltpu.roll(jnp.where(group == 3, low, zrow[k, 1, x]), 32, 1)
            zmix[1, x] = pltpu.roll(jnp.where(group == 0, top, zrow[k, 0, x]), 96, 1)

        def plane(x):
            packed = (jnp.zeros((8, 128), F32),) * 2
            for y in range(8):
                c = [field[k, x + 1, y + 1, SPANS[b], :] for b in range(4)]
                ups = [pltpu.roll(v, 1, 0) for v in c]
                downs = [pltpu.roll(v, 7, 0) for v in c]
                new = []
                for b in range(4):
                    before = zmix[0, x, y : y + 1, :] if b == 0 else ups[b - 1]
                    after = zmix[1, x, y : y + 1, :] if b == 3 else downs[b + 1]
                    up = jnp.where(sub == 0, before, ups[b])
                    down = jnp.where(sub == 7, after, downs[b])
                    sp = SPANS[b]
                    around = (
                        (field[k, x, y + 1, sp, :] + field[k, x + 2, y + 1, sp, :])
                        + (field[k, x + 1, y, sp, :] + field[k, x + 1, y + 2, sp, :])
                        + (up + down)
                    )
                    new.append(
                        (1.0 - factor) * c[b]
                        + factor * (base[x, y, sp, :] + conduct[x, y, sp, :] * around)
                    )
                if seen is not None:
                    for b in range(4):
                        seen[x, y, SPANS[b], :] = new[b]
                if not last:
                    packed = keep(k + 1, x, y, new, packed)
            if not last:
                zrow[k + 1, 0, x], zrow[k + 1, 1, x] = packed

        if last:
            pl.loop(0, 8)(plane)
        else:
            ends_first(plane, lambda: halo_start(k + 1, (0, 1)))
            pack_rows(k + 1)
            if seen is None:
                halo_start(k + 1, (4, 5, 2, 3))

    def send_flux(it, ref):
        for s in range(SLOTS):
            place = cells[s]
            picked[s : s + 1, :] = ref[
                place >> 8, (place >> 5) & 7, pl.ds(place & 31, 1), :
            ]
        fluxes = []
        for p in range(2):
            seen = picked[8 * p : 8 * p + 8, :] * mine[p]
            seen = seen + pltpu.roll(seen, 64, 1)
            seen = seen + pltpu.roll(seen, 32, 1)
            fluxes.append(seen - slot[p])
        fsend[it] = jnp.where(group % 2 == 0, fluxes[0], fluxes[1])
        fbuf[it, me] = fsend[it]

        @pl.loop(1, blocks)
        def _(d):
            remote(
                fsend.at[it], fbuf.at[it, me], phase_send.at[2 + it], phase_recv.at[2 + it],
                block_id(block_peer(d)),
            ).start()

    def spread_flux(it):
        whole(fbuf.at[it, pl.ds(0, blocks - 1)], 2 + it).wait_recv()
        seen = fbuf[it].reshape(blocks * 8, 128).astype(BF16)
        dense = jnp.zeros((lead, 128), F32)
        for p in range(2):
            half = select[p * blocks * 8 : (p + 1) * blocks * 8, :]
            every = lax.dot_general(seen, half, TN, preferred_element_type=F32)
            dense += every[lead * p : lead * p + lead, :]
        fall[it, mine_near] = dense.astype(BF16)
        for peer in nears:
            remote(
                fall.at[it, mine_near], fall.at[it, mine_near], phase_send.at[4 + it],
                phase_recv.at[4 + it], {"row": peer},
            ).start()

    def new_share(it, old):
        whole(fall.at[it, pl.ds(0, near - 1)], 4 + it).wait_recv()
        if it == 0:
            whole(strip.at[pl.ds(0, near - 1)], 6).wait_recv()
        for f in range(far):
            update = jnp.zeros((lead, share), F32)
            for n in range(near):
                update += jnp.dot(fall[it, n], strip[n, f], preferred_element_type=F32)
            usend[it, f] = update
        urecv[it, mine_far] = usend[it, mine_far]
        for d in range(1, far):
            f = lax.rem(mine_far + d, far)
            remote(
                usend.at[it, f], urecv.at[it, mine_far], phase_send.at[7 + it],
                phase_recv.at[7 + it], {"row": lax.rem(row + near * d, n_row)},
            ).start()
        if far > 1:
            whole(urecv.at[it, pl.ds(0, far - 1)], 7 + it).wait_recv()
        update = urecv[it, 0]
        for f in range(1, far):
            update += urecv[it, f]
        return old + RELAXATION * update

    right_side(0)
    first_sweep(0, factors[0])
    send_panel(1)
    sweep(0, factors[1], False)
    send_panel(2)
    sweep(1, factors[2], False)
    send_panel(3)
    sweep(2, factors[3], False, middle)
    send_flux(0, middle)
    halo_start(3, (4, 5, 2, 3))
    spread_flux(0)
    state = new_share(0, density[:, own])
    osend[0] = state
    rbuf[row] = state.astype(BF16)

    sent_rounded = gather(0, lambda r: rbuf.at[r])

    send_potential(1, lambda k: rbuf[k])
    right_side(1)
    sweep(3, factors[0], False)
    sweep(4, factors[1], False)
    sweep(5, factors[2], False)
    sweep(6, factors[3], True, inner)
    send_flux(1, inner)

    @pl.loop(0, 16, unroll=TURN)
    def _(i):
        x, y = i // 2, (i % 2) * 4
        tiles = quarters([inner[x, y + q] for q in range(4)])
        back = jnp.transpose(jnp.concatenate(tiles, axis=0))
        for q in range(4):
            volume_out[pl.ds(x * 8 + y + q, lead, stride=64), :] = back[lead * q : lead * q + lead, :]

    spread_flux(1)
    state = new_share(1, osend[0])
    density_out[:, own] = state

    sent_final = gather(
        1, lambda r: density_out.at[:, pl.ds(pl.multiple_of(r * share, share), share)]
    )

    for it in range(OUTER):
        whole(pbuf.at[it, pl.ds(0, blocks - 1)], it).wait_send()
        whole(fbuf.at[it, pl.ds(0, blocks - 1)], 2 + it).wait_send()
        whole(fall.at[it, pl.ds(0, near - 1)], 4 + it).wait_send()
        if far > 1:
            whole(urecv.at[it, pl.ds(0, far - 1)], 7 + it).wait_send()
    whole(strip.at[pl.ds(0, near - 1)], 6).wait_send()
    sent_rounded()
    sent_final()
    for k in range(exchanges):
        halo_sent(k)


def local(panel, density, source, class_index, class_values, trace_count, trace_cell):
    sizes = (lax.axis_size("row"), lax.axis_size("col"), lax.axis_size("vol"))
    n_row, n_col, n_vol = sizes
    blocks = n_col * n_vol
    lead = source.shape[0]
    targets, nodes = panel.shape
    share = nodes // n_row
    near = min(4, n_row)
    ex = SWEEPS * OUTER - 1
    vmem = lambda shape, kind=F32: pltpu.VMEM(shape, kind)
    dma = pltpu.SemaphoreType.DMA
    density_out, volume = pl.pallas_call(
        functools.partial(kernel, sizes),
        out_shape=(
            jax.ShapeDtypeStruct(density.shape, F32),
            jax.ShapeDtypeStruct((lead * 64, 128), F32),
        ),
        in_specs=[pl.BlockSpec(memory_space=pltpu.VMEM)] * 4
        + [pl.BlockSpec(memory_space=pltpu.SMEM)] * 3,
        out_specs=(pl.BlockSpec(memory_space=pltpu.VMEM),) * 2,
        scratch_shapes=[
            vmem((blocks * SLOTS, targets), BF16),
            vmem((2048, 128), BF16),
            vmem((8, 8, 32, 128)),
            vmem((8, 8, 32, 128)),
            vmem((8, 8, 32, 128)),
            vmem((8, 8, 32, 128)),
            vmem((8, 8, 32, 128)),
            vmem((ex, 10, 10, 32, 128)),
            vmem((ex, 2, 2, 8, 128)),
            vmem((ex, 2, 8, 128)),
            vmem((ex, 2, 8, 128)),
            vmem((ex, 2, 8, 8, 128)),
            vmem((2, 8, 8, 128)),
            vmem((64, 128)),
            vmem((2, 8, 128)),
            vmem((SLOTS, 128)),
            vmem((OUTER, blocks, 8, 128)),
            vmem((OUTER, blocks, 8, 128)),
            vmem((OUTER, 8, 128)),
            vmem((OUTER, blocks, 8, 128)),
            vmem((OUTER, near, lead, targets), BF16),
            vmem((near, n_row // near, targets, share), BF16),
            vmem((OUTER, n_row // near, lead, share)),
            vmem((OUTER, n_row // near, lead, share)),
            vmem((n_row, lead, share), BF16),
            vmem((1, lead, share)),
            dma((ex, 6)),
            dma((ex, 6)),
            dma((9,)),
            dma((9,)),
            dma((2, n_row, n_row)),
            dma((2, n_row)),
        ],
        compiler_params=pltpu.CompilerParams(
            collective_id=0, has_side_effects=True, vmem_limit_bytes=56 * 1024 * 1024
        ),
    )(
        panel,
        density,
        source.reshape(lead * 64, 128),
        class_index.reshape(64, 128),
        class_values,
        trace_count,
        trace_cell,
    )
    return density_out, volume.reshape(source.shape)


def solution(mesh):
    placed = (
        P("row", ("col", "vol")),
        P(None, ("col", "vol")),
        P(None, "row", "col", "vol"),
        P("row", "col", "vol"),
        P(),
        P("row", None),
        P("row", None, None),
    )
    return jax.shard_map(
        local,
        mesh=mesh,
        in_specs=placed,
        out_specs=(P(None, ("col", "vol")), P(None, "row", "col", "vol")),
        check_vma=False,
    )
```
